256 devices in a mesh: gx: 8 (over z), gz: 4 (over x), gy: 8 (over y, core).
Axes of the slice: x: 4, y: 4, z: 8, core: 2. Of those that a mesh axis runs over, the one named last changes fastest.
Arguments:
- row_embed: bfloat16 [131072, 128], P(('gx', 'gz')), may hold values from -24 to 24, as said below
- col_embed: bfloat16 [4096, 128], P('gy'), may hold values from -24 to 24, as said below
- row_mass: float32 [131072], P(('gx', 'gz')), may hold values from 1 to 10
- col_mass: float32 [4096], P('gy'), may hold values from 1 to 10
Outputs:
- row_potential: float32 [131072], P(('gx', 'gz'))
- col_potential: float32 [4096], P('gy')
- errors: float32 [10, 2], replicated
The draws below stay inside these ranges and needn't reach their ends.
Inputs may be any that keep to these rules, and one draw needn't show every extreme that they name: `row_embed`: entries are real-valued embedding coordinates. `col_embed`: entries are real-valued embedding coordinates.
All inputs are finite; a program needn't handle non-finite values.
Results may differ from the reference program's by a relative error of at most 0.0003.
Values sent between devices are 32-bit elements; how exact they have to be, the bound alone decides.
No kernel may reach another device: no remote copies, remote signals or barrier semaphores. Data moves between devices by JAX's collectives and lax.ppermute only.
A program may use at most 64 MiB of HBM per device.

```python
import math
import jax
import jax.numpy as jnp
from jax import lax

E = 128
ITERS = 10
NR = 131072
NC = 4096


def embed_draw(key, count):
    base = jnp.clip(jax.random.normal(jax.random.fold_in(key, 11), (count, E), jnp.float32), -6.0, 6.0)
    return base.astype(jnp.bfloat16)


def draw_row_embed(key, part):
    return embed_draw(jax.random.fold_in(key, 1), NR)


def draw_col_embed(key, part):
    return embed_draw(jax.random.fold_in(key, 2), NC)


def block_levels(rng, dims, cuts, smallest, top_value):
    gain, own = 1.0, jax.random.fold_in(rng, 6)
    for dim, parts in cuts:
        steps = jnp.exp(jax.random.uniform(jax.random.fold_in(own, dim), (parts,), jnp.float32, smallest / len(cuts), top_value / len(cuts)))
        gain = gain * jnp.repeat(steps, dims[dim] // parts).reshape([-1 if axis == dim else 1 for axis in range(len(dims))])
    return gain


def setup_inputs(seed: int = 0) -> dict:
    seeds = jax.random.split(jax.random.key(seed), 5)
    return {
        "row_embed": draw_row_embed(jax.random.fold_in(seeds[4], 71), 0),
        "col_embed": draw_col_embed(jax.random.fold_in(seeds[4], 71), 0),
        "row_mass": jnp.clip(jnp.exp(math.log(10.0) - 2.3025851 * jax.random.uniform(seeds[2], (NR,), jnp.float32) ** block_levels(seeds[2], (NR,), ((0, 32),), -0.2, 0.2)), 1.0, 10.0),
        "col_mass": jnp.clip(jnp.exp(math.log(10.0) - 2.3025851 * jax.random.uniform(seeds[3], (NC,), jnp.float32) ** block_levels(seeds[3], (NC,), ((0, 8),), -0.2, 0.2)), 1.0, 10.0),
    }


eps = 0.05


def cost_block(xb, col_embed, col_sq):
    cross = jnp.dot(xb, col_embed.T, preferred_element_type=jnp.float32)
    xf = xb.astype(jnp.float32)
    row_sq = jnp.sum(xf * xf, axis=1)
    return (row_sq[:, None] + col_sq[None, :] - 2.0 * cross) / E


def reference(row_embed, col_embed, row_mass, col_mass):
    mass_a = row_mass / jnp.sum(row_mass)
    mass_b = col_mass / jnp.sum(col_mass)
    log_a = jnp.log(mass_a)
    log_b = jnp.log(mass_b)
    yf = col_embed.astype(jnp.float32)
    col_sq = jnp.sum(yf * yf, axis=1)
    block = math.gcd(NR, 2048)
    count = NR // block
    xblocks = row_embed.reshape(count, block, E)

    def row_lse(g_pot):
        def one(xb):
            z = (g_pot[None, :] - cost_block(xb, col_embed, col_sq)) / eps
            top = jnp.max(z, axis=1)
            return top + jnp.log(jnp.sum(jnp.exp(z - top[:, None]), axis=1))
        return lax.map(one, xblocks).reshape(NR)

    def col_lse(f_pot):
        fblocks = f_pot.reshape(count, block)

        def step(carry, item):
            top, total = carry
            xb, fb = item
            z = (fb[:, None] - cost_block(xb, col_embed, col_sq)) / eps
            newtop = jnp.maximum(top, jnp.max(z, axis=0))
            total = total * jnp.exp(top - newtop) + jnp.sum(jnp.exp(z - newtop[None, :]), axis=0)
            return (newtop, total), None
        start = (jnp.full((NC,), -jnp.inf, jnp.float32), jnp.zeros((NC,), jnp.float32))
        (top, total), unused = lax.scan(step, start, (xblocks, fblocks))
        return top + jnp.log(total)

    f_pot = jnp.zeros((NR,), jnp.float32)
    g_pot = jnp.zeros((NC,), jnp.float32)
    rows_out = []
    for index in range(ITERS):
        f_new = eps * (log_a - row_lse(g_pot))
        rows_out.append(jnp.sum(jnp.abs(jnp.exp(log_a + (f_pot - f_new) / eps) - mass_a)))
        f_pot = f_new
        g_new = eps * (log_b - col_lse(f_pot))
        rows_out.append(jnp.sum(jnp.abs(jnp.exp(log_b + (g_pot - g_new) / eps) - mass_b)))
        g_pot = g_new
    errors = jnp.stack(rows_out).reshape(ITERS, 2)
    return f_pot, g_pot, errors
```

```python
import functools
import math

import jax
import jax.numpy as jnp
from jax import lax
from jax.experimental import pallas as pl
from jax.experimental.pallas import tpu as pltpu
from jax.sharding import PartitionSpec as P

ITERS = 10
ROWS_OVER = ("gx", "gz")
COLS_OVER = "gy"
eps = 0.05
LOG2E = 1.0 / math.log(2.0)
LANES = 128
SMALLEST = 1e-26
f32 = jnp.float32


def log2(x):
    return jnp.log(x) * LOG2E


def lane_and_sublane():
    return (
        lax.broadcasted_iota(jnp.int32, (8, LANES), 1),
        lax.broadcasted_iota(jnp.int32, (8, LANES), 0),
    )


def total(x):
    return jnp.sum(jnp.sum(x, axis=1, keepdims=True), axis=0, keepdims=True)


def largest(x):
    return jnp.max(jnp.max(x, axis=1, keepdims=True), axis=0, keepdims=True)


def scaled_norms(embed, kappa):
    wide = embed.astype(f32)
    return kappa * jnp.sum(wide * wide, axis=1, keepdims=True)


def cross_of(y, xb):
    return lax.dot_general(y, xb, (((1,), (1,)), ((), ())), preferred_element_type=f32)


def joined(pieces):
    count = len(pieces)
    top = pieces[0]
    for k in range(1, count):
        top = jnp.maximum(top, pieces[k])
    weight = jnp.exp2(pieces[0] - top)
    for k in range(1, count):
        weight = weight + jnp.exp2(pieces[k] - top)
    return top + log2(weight)


def column_form(line, put):
    lane, sub = lane_and_sublane()
    for t in range(line.shape[0]):
        for q in range(LANES // 8):
            picked = jnp.where(lane == sub + 8 * q, line[t : t + 1, :], 0.0)
            put(t * LANES + 8 * q, jnp.broadcast_to(jnp.sum(picked, axis=1, keepdims=True), (8, LANES)))


def spread(out_ref, lines, extra):
    rows = lines.shape[0]
    for d in range(out_ref.shape[0]):
        out_ref[d, 0:rows, :] = lines
        if extra is not None:
            out_ref[d, rows : rows + extra.shape[0], :] = extra


def init_kernel(kappa, x_ref, y_ref, cm_ref, k_ref, mr_ref, xs_ref, out_ref, cs_ref, l_ref):
    cols = y_ref.shape[0]
    rows = x_ref.shape[0]
    wide = 512
    cs_ref[...] = jnp.broadcast_to(scaled_norms(y_ref[...], kappa), (cols, LANES))
    ones = jnp.ones((8, x_ref.shape[1]), f32)

    def chunk(c, carry):
        at = pl.multiple_of(c * wide, wide)
        xb = x_ref[pl.ds(at, wide), :]
        k_ref[:, pl.ds(at, wide)] = cross_of(y_ref[...], xb) * (2.0 * kappa)
        xf = xb.astype(f32)
        norms = kappa * lax.dot_general(
            ones, xf * xf, (((1,), (1,)), ((), ())),
            precision=lax.Precision.HIGHEST, preferred_element_type=f32,
        )
        for t in range(wide // LANES):
            here = pl.ds(pl.multiple_of(at + t * LANES, LANES), LANES)
            tops = [None] * 4
            for j in range(cols // 8):
                z = k_ref[8 * j : 8 * j + 8, here] - cs_ref[8 * j : 8 * j + 8, :]
                tops[j % 4] = z if tops[j % 4] is None else jnp.maximum(tops[j % 4], z)
            top = jnp.maximum(jnp.maximum(tops[0], tops[1]), jnp.maximum(tops[2], tops[3]))
            top = jnp.max(top, axis=0, keepdims=True)
            sums = [None] * 4
            for j in range(cols // 8):
                e = jnp.exp2(k_ref[8 * j : 8 * j + 8, here] - cs_ref[8 * j : 8 * j + 8, :] - top)
                k_ref[8 * j : 8 * j + 8, here] = e
                sums[j % 4] = e if sums[j % 4] is None else sums[j % 4] + e
            weight = jnp.sum((sums[0] + sums[1]) + (sums[2] + sums[3]), axis=0, keepdims=True)
            norm = norms[0:1, t * LANES : (t + 1) * LANES]
            line = pl.ds(c * (wide // LANES) + t, 1)
            xs_ref[line, :] = norm
            mr_ref[line, :] = top - norm
            l_ref[line, :] = (top - norm) + log2(weight)
        return carry

    lax.fori_loop(0, rows // wide, chunk, 0)
    mass = jnp.broadcast_to(jnp.sum(cm_ref[...], axis=0, keepdims=True), (8, LANES))
    spread(out_ref, l_ref[...], mass)


def exact_rows(kappa, x_ref, y_ref, gcol_ref, xs_ref, l_ref):
    cols = y_ref.shape[0]
    cs = scaled_norms(y_ref[...], kappa)

    def chunk(c, carry):
        at = pl.multiple_of(c * LANES, LANES)
        z = cross_of(y_ref[...], x_ref[pl.ds(at, LANES), :]) * (2.0 * kappa) - cs + gcol_ref[...]
        top = jnp.max(z, axis=0, keepdims=True)
        weight = jnp.sum(jnp.exp2(z - top), axis=0, keepdims=True)
        l_ref[pl.ds(c, 1), :] = top - xs_ref[pl.ds(c, 1), :] + log2(weight)
        return carry

    lax.fori_loop(0, x_ref.shape[0] // LANES, chunk, 0)


def exact_cols(kappa, x_ref, y_ref, fx_ref, s_ref, top_ref, weight_ref):
    cols = y_ref.shape[0]
    top_ref[...] = jnp.full(top_ref.shape, -jnp.inf, f32)
    weight_ref[...] = jnp.zeros(weight_ref.shape, f32)

    def chunk(c, carry):
        at = pl.multiple_of(c * LANES, LANES)
        z = cross_of(y_ref[...], x_ref[pl.ds(at, LANES), :]) * (2.0 * kappa) + fx_ref[pl.ds(c, 1), :]
        top = top_ref[...]
        newtop = jnp.maximum(top, jnp.max(z, axis=1, keepdims=True))
        weight_ref[...] = weight_ref[...] * jnp.exp2(top - newtop) + jnp.sum(
            jnp.exp2(z - newtop), axis=1, keepdims=True
        )
        top_ref[...] = newtop
        return carry

    lax.fori_loop(0, x_ref.shape[0] // LANES, chunk, 0)
    lse = top_ref[...] + log2(weight_ref[...]) - scaled_norms(y_ref[...], kappa)
    lane, sub = lane_and_sublane()
    for t in range(cols // LANES):
        line = jnp.zeros((8, LANES), f32)
        for q in range(LANES // 8):
            at = t * LANES + 8 * q
            line = line + jnp.where(lane == sub + 8 * q, lse[at : at + 8, :], 0.0)
        s_ref[t : t + 1, :] = jnp.sum(line, axis=0, keepdims=True)


def col_kernel(
    kappa, index, last,
    recv_ref, rm_ref, fprev_ref, mr_ref, xs_ref, sc_ref, errs_ref, k_ref, x_ref, y_ref,
    f_ref, sc_out_ref, errs_out_ref, out_ref,
    ubc_ref, s_ref, fx_ref, top_ref, weight_ref,
):
    rows, cols = k_ref.shape[1], k_ref.shape[0]
    lines = rows // LANES
    lane, sub = lane_and_sublane()
    lse = joined([recv_ref[d, 0:lines, :] for d in range(recv_ref.shape[0])])
    mass = rm_ref[...]
    la = log2(mass)
    sc = sc_ref[...]
    errs = errs_ref[...]
    if index == 0:
        f_new = la - lse
        mass_b = total(jnp.sum(recv_ref[:, lines : lines + 1, :], axis=0))
        sc_out_ref[...] = jnp.where(sub == 1, mass_b, 0.0)
        errs_out_ref[...] = errs
    else:
        mass_a = jnp.max(sc[0:1, :], axis=1, keepdims=True)
        shift = log2(mass_a)
        f_new = la - shift - lse
        share = mass / mass_a
        if index == 1:
            old = total(jnp.abs(jnp.exp2(la - fprev_ref[...]) - share))
            errs = jnp.where(lane == 0, old, errs)
            f_old = fprev_ref[...] - shift
        else:
            f_old = fprev_ref[...]
        now = total(jnp.abs(jnp.exp2(la - shift + (f_old - f_new)) - share))
        errs = jnp.where(lane == index, now, errs)
        sc_out_ref[...] = sc
        errs_out_ref[...] = errs
    f_ref[...] = f_new
    u = f_new + mr_ref[...]
    high = largest(u)
    u = jnp.exp2(u - high)
    for l in range(lines):
        ubc_ref[:, l * LANES : (l + 1) * LANES] = jnp.broadcast_to(u[l : l + 1, :], (8, LANES))

    def group(t, carry):
        line = jnp.zeros((8, LANES), f32)
        for half in range(2):
            acc = [None] * 8
            for l in range(lines):
                across = slice(l * LANES, (l + 1) * LANES)
                ul = ubc_ref[:, across]
                for q in range(8):
                    at = pl.multiple_of(t * LANES + half * 64 + 8 * q, 8)
                    term = k_ref[pl.ds(at, 8), across] * ul
                    acc[q] = term if acc[q] is None else acc[q] + term
            for q in range(8):
                full = jnp.sum(acc[q], axis=1, keepdims=True)
                line = line + jnp.where(lane == sub + (half * 64 + 8 * q), full, 0.0)
        s_ref[pl.ds(t, 1), :] = jnp.sum(line, axis=0, keepdims=True)
        return carry

    lax.fori_loop(0, cols // LANES, group, 0)
    sums = s_ref[...]
    least = jnp.min(sums)
    s_ref[...] = high + log2(sums)

    @pl.when(jnp.logical_not(least >= SMALLEST))
    def _():
        fx_ref[...] = f_new - xs_ref[...]
        exact_cols(kappa, x_ref, y_ref, fx_ref, s_ref, top_ref, weight_ref)

    extra = None
    if index == 0:
        extra = jnp.broadcast_to(jnp.sum(mass, axis=0, keepdims=True), (4, LANES))
    elif last:
        extra = errs[0:4, :]
    spread(out_ref, s_ref[...], extra)


def new_target(index, recv_ref, cm_ref, gprev_ref, sc_ref, errs_ref):
    lines = cm_ref.shape[0]
    lane, sub = lane_and_sublane()
    lse = joined([recv_ref[d, 0:lines, :] for d in range(recv_ref.shape[0])])
    sc = sc_ref[...]
    mass_b = jnp.max(sc[1:2, :], axis=1, keepdims=True)
    if index == 0:
        mass_a = total(jnp.sum(recv_ref[:, lines : lines + 1, :], axis=0))
        lse = lse - log2(mass_a)
        sc = jnp.where(sub == 0, mass_a, sc)
    mass = cm_ref[...]
    lb = log2(mass) - log2(mass_b)
    g_new = lb - lse
    now = total(jnp.abs(jnp.exp2(lb + (gprev_ref[...] - g_new)) - mass / mass_b))
    errs = jnp.where(lane == index, now, errs_ref[...])
    return g_new, sc, errs


def row_kernel(
    kappa, index,
    recv_ref, cm_ref, gprev_ref, mr_ref, xs_ref, sc_ref, errs_ref, k_ref, x_ref, y_ref,
    g_ref, sc_out_ref, errs_out_ref, out_ref,
    vbc_ref, r_ref, l_ref,
):
    rows, cols = k_ref.shape[1], k_ref.shape[0]
    g_new, sc, errs = new_target(index, recv_ref, cm_ref, gprev_ref, sc_ref, errs_ref)
    g_ref[...] = g_new
    sc_out_ref[...] = sc
    errs_out_ref[...] = errs
    high = largest(g_new)

    def put(at, piece):
        vbc_ref[at : at + 8, :] = piece

    column_form(jnp.exp2(g_new - high), put)
    together = 8

    def group(c, carry):
        acc = [None] * together
        for j in range(cols // 8):
            vj = vbc_ref[8 * j : 8 * j + 8, :]
            for t in range(together):
                at = pl.multiple_of(c * (together * LANES) + t * LANES, LANES)
                term = k_ref[8 * j : 8 * j + 8, pl.ds(at, LANES)] * vj
                acc[t] = term if acc[t] is None else acc[t] + term
        for t in range(together):
            r_ref[pl.ds(c * together + t, 1), :] = jnp.sum(acc[t], axis=0, keepdims=True)
        return carry

    lax.fori_loop(0, rows // (together * LANES), group, 0)
    sums = r_ref[...]
    least = jnp.min(sums)
    l_ref[...] = mr_ref[...] + (high + log2(sums))

    @pl.when(jnp.logical_not(least >= SMALLEST))
    def _():
        column_form(g_new, put)
        exact_rows(kappa, x_ref, y_ref, vbc_ref, xs_ref, l_ref)

    spread(out_ref, l_ref[...], None)


def last_kernel(
    index, recv_ref, cm_ref, gprev_ref, sc_ref, errs_ref, g_ref, row_ref, out_ref
):
    lines = cm_ref.shape[0]
    g_new, sc, errs = new_target(index, recv_ref, cm_ref, gprev_ref, sc_ref, errs_ref)
    g_ref[...] = g_new * (eps / LOG2E)
    row_ref[...] = jnp.broadcast_to(jnp.sum(recv_ref[:, lines : lines + 1, :], axis=0), (8, LANES))
    for d in range(out_ref.shape[0]):
        out_ref[d] = errs


def on_chip():
    return pl.BlockSpec(memory_space=pltpu.VMEM)


def call(kernel, args, outs, scratch, limit, name):
    return pl.pallas_call(
        kernel,
        in_specs=[on_chip() for _ in args],
        out_specs=[on_chip() for _ in outs],
        out_shape=[jax.ShapeDtypeStruct(shape, f32) for shape in outs],
        scratch_shapes=[pltpu.VMEM(shape, f32) for shape in scratch],
        compiler_params=pltpu.CompilerParams(vmem_limit_bytes=limit),
        name=name,
    )(*args)


def exchange(x, axis):
    return lax.all_to_all(x, axis, split_axis=0, concat_axis=0, tiled=True)


def on_device(row_embed, col_embed, row_mass, col_mass):
    rows, width = row_embed.shape
    cols = col_embed.shape[0]
    kappa = LOG2E / (width * eps)
    row_lines, col_lines = rows // LANES, cols // LANES
    by_col = lax.axis_size(COLS_OVER)
    by_row = lax.axis_size(ROWS_OVER)
    rm = row_mass.reshape(row_lines, LANES)
    cm = col_mass.reshape(col_lines, LANES)
    tile = (8, LANES)
    mib = 1 << 20
    k, mr, xs, out = call(
        functools.partial(init_kernel, kappa),
        (row_embed, col_embed, cm),
        [(cols, rows), (row_lines, LANES), (row_lines, LANES), (by_col, row_lines + 8, LANES)],
        [(cols, LANES), (row_lines, LANES)],
        24 * mib, "init",
    )
    f_pot = jnp.zeros((row_lines, LANES), f32)
    g_pot = jnp.zeros((col_lines, LANES), f32)
    sc = jnp.zeros(tile, f32)
    row_errs = jnp.zeros(tile, f32)
    col_errs = jnp.zeros(tile, f32)
    for index in range(ITERS):
        last = index == ITERS - 1
        got = exchange(out, COLS_OVER)
        more = 4 if index == 0 or last else 0
        f_pot, sc, row_errs, out = call(
            functools.partial(col_kernel, kappa, index, last),
            (got, rm, f_pot, mr, xs, sc, row_errs, k, row_embed, col_embed),
            [(row_lines, LANES), tile, tile, (by_row, col_lines + more, LANES)],
            [(8, rows), (col_lines, LANES), (row_lines, LANES), (cols, LANES), (cols, LANES)],
            24 * mib, f"cols{index}",
        )
        got = exchange(out, ROWS_OVER)
        if last:
            break
        g_pot, sc, col_errs, out = call(
            functools.partial(row_kernel, kappa, index),
            (got, cm, g_pot, mr, xs, sc, col_errs, k, row_embed, col_embed),
            [(col_lines, LANES), tile, tile, (by_col, row_lines, LANES)],
            [(cols, LANES), (row_lines, LANES), (row_lines, LANES)],
            24 * mib, f"rows{index}",
        )
    g_out, row_errs, out = call(
        functools.partial(last_kernel, ITERS - 1),
        (got, cm, g_pot, sc, col_errs),
        [(col_lines, LANES), tile, (by_col, 8, LANES)],
        [], 8 * mib, "finish",
    )
    got = exchange(out, COLS_OVER)
    col_vec = jnp.sum(got[:, 0, :ITERS], axis=0)
    errors = jnp.stack([row_errs[0, :ITERS], col_vec], axis=1)
    f_out = f_pot * (eps / LOG2E)
    return f_out.reshape(rows), g_out.reshape(cols), errors


def solution(mesh):
    return jax.shard_map(
        on_device,
        mesh=mesh,
        in_specs=(P(ROWS_OVER, None), P(COLS_OVER, None), P(ROWS_OVER), P(COLS_OVER)),
        out_specs=(P(ROWS_OVER), P(COLS_OVER), P()),
        check_vma=False,
    )
```

```python
import functools
import math

import jax
import jax.numpy as jnp
from jax import lax
from jax.experimental import pallas as pl
from jax.experimental.pallas import tpu as pltpu
from jax.sharding import PartitionSpec as P

ITERS = 10
ROWS_OVER = ("gx", "gz")
COLS_OVER = "gy"
eps = 0.05
LOG2E = 1.0 / math.log(2.0)
LANES = 128
SMALLEST = 1e-20
DRIFT = 20.0
f32 = jnp.float32


def log2(x):
    return jnp.log(x) * LOG2E


def lane_and_sublane():
    return (
        lax.broadcasted_iota(jnp.int32, (8, LANES), 1),
        lax.broadcasted_iota(jnp.int32, (8, LANES), 0),
    )


def total(x):
    return jnp.sum(jnp.sum(x, axis=1, keepdims=True), axis=0, keepdims=True)


def largest(x):
    return jnp.max(jnp.max(x, axis=1, keepdims=True), axis=0, keepdims=True)


def scaled_norms(embed, kappa):
    wide = embed.astype(f32)
    return kappa * jnp.sum(wide * wide, axis=1, keepdims=True)


def cross_of(y, xb):
    return lax.dot_general(y, xb, (((1,), (1,)), ((), ())), preferred_element_type=f32)


def in_pairs(pieces, combine):
    while len(pieces) > 1:
        rest = [pieces[-1]] if len(pieces) % 2 else []
        pieces = [combine(*pair) for pair in zip(pieces[::2], pieces[1::2])] + rest
    return pieces[0]


def joined(pieces):
    top = in_pairs(pieces, jnp.maximum)
    return top + log2(in_pairs([jnp.exp2(piece - top) for piece in pieces], jnp.add))


def column_form(line, put):
    lane, sub = lane_and_sublane()
    for t in range(line.shape[0]):
        for q in range(LANES // 8):
            picked = jnp.where(lane == sub + 8 * q, line[t : t + 1, :], 0.0)
            put(t * LANES + 8 * q, jnp.broadcast_to(jnp.sum(picked, axis=1, keepdims=True), (8, LANES)))


def spread(out_ref, lines, extra):
    rows = lines.shape[0]
    for d in range(out_ref.shape[0]):
        out_ref[d, 0:rows, :] = lines
        if extra is not None:
            out_ref[d, rows : rows + extra.shape[0], :] = extra


def noted(errs, index, terms):
    row = lax.broadcasted_iota(jnp.int32, errs.shape, 0)
    return jnp.where(row == index, jnp.sum(terms, axis=0, keepdims=True), errs)


def along_lanes(errs):
    row = lax.broadcasted_iota(jnp.int32, errs.shape, 0)
    lane = lax.broadcasted_iota(jnp.int32, errs.shape, 1)
    picked = jnp.where(row == lane, jnp.sum(errs, axis=1, keepdims=True), 0.0)
    return jnp.sum(picked, axis=0, keepdims=True)


def init_kernel(
    kappa, x_hbm, y_hbm, rm_hbm, cm_hbm,
    x_ref, y_ref, rm_ref, cm_ref, k_ref, mr_ref, xs_ref, out_ref, half_ref, l_ref, sems,
):
    pairs = ((y_hbm, y_ref), (x_hbm, x_ref), (cm_hbm, cm_ref), (rm_hbm, rm_ref))
    copies = [pltpu.make_async_copy(src, dst, sems.at[i]) for i, (src, dst) in enumerate(pairs)]
    for copy in copies:
        copy.start()
    cols = y_ref.shape[0]
    rows = x_ref.shape[0]
    wide, block = 512, 64
    tiles = wide // LANES
    copies[0].wait()
    half_ref[...] = jnp.broadcast_to(scaled_norms(y_ref[...], 0.5), (cols, LANES))
    ones = jnp.ones((8, x_ref.shape[1]), f32)
    copies[1].wait()

    def chunk(c, carry):
        at = pl.multiple_of(c * wide, wide)
        xb = x_ref[pl.ds(at, wide), :]
        k_ref[:, pl.ds(at, wide)] = cross_of(y_ref[...], xb)
        xf = xb.astype(f32)
        norms = kappa * lax.dot_general(
            ones, xf * xf, (((1,), (1,)), ((), ())),
            precision=lax.Precision.HIGHEST, preferred_element_type=f32,
        )
        here = [pl.ds(pl.multiple_of(at + t * LANES, LANES), LANES) for t in range(tiles)]

        def highest(b, tops):
            tops = list(tops)
            for j in range(block // 8):
                line = pl.ds(pl.multiple_of(b * block + 8 * j, 8), 8)
                half = half_ref[line, :]
                for t in range(tiles):
                    z = k_ref[line, here[t]] - half
                    k_ref[line, here[t]] = z
                    tops[t] = jnp.maximum(tops[t], z)
            return tuple(tops)

        low = jnp.full((8, LANES), -jnp.inf, f32)
        tops = lax.fori_loop(0, cols // block, highest, (low,) * tiles)
        tops = [jnp.max(top, axis=0, keepdims=True) for top in tops]
        spans = [jnp.broadcast_to(top, (8, LANES)) for top in tops]

        def weigh(b, sums):
            sums = list(sums)
            for j in range(block // 8):
                line = pl.ds(pl.multiple_of(b * block + 8 * j, 8), 8)
                for t in range(tiles):
                    e = jnp.exp2((k_ref[line, here[t]] - spans[t]) * (2.0 * kappa))
                    k_ref[line, here[t]] = e
                    sums[t] = sums[t] + e
            return tuple(sums)

        sums = lax.fori_loop(0, cols // block, weigh, (jnp.zeros((8, LANES), f32),) * tiles)
        for t in range(tiles):
            weight = jnp.sum(sums[t], axis=0, keepdims=True)
            norm = norms[0:1, t * LANES : (t + 1) * LANES]
            line = pl.ds(c * tiles + t, 1)
            base = tops[t] * (2.0 * kappa) - norm
            xs_ref[line, :] = norm
            mr_ref[line, :] = base
            l_ref[line, :] = base + log2(weight)
        return carry

    lax.fori_loop(0, rows // wide, chunk, 0)
    copies[2].wait()
    copies[3].wait()
    mass = jnp.broadcast_to(jnp.sum(cm_ref[...], axis=0, keepdims=True), (8, LANES))
    spread(out_ref, l_ref[...], mass)


def exact_rows(kappa, x_ref, y_ref, gcol_ref, xs_ref, l_ref):
    cols = y_ref.shape[0]
    cs = scaled_norms(y_ref[...], kappa)

    def chunk(c, carry):
        at = pl.multiple_of(c * LANES, LANES)
        z = cross_of(y_ref[...], x_ref[pl.ds(at, LANES), :]) * (2.0 * kappa) - cs + gcol_ref[...]
        top = jnp.max(z, axis=0, keepdims=True)
        weight = jnp.sum(jnp.exp2(z - top), axis=0, keepdims=True)
        l_ref[pl.ds(c, 1), :] = top - xs_ref[pl.ds(c, 1), :] + log2(weight)
        return carry

    lax.fori_loop(0, x_ref.shape[0] // LANES, chunk, 0)


def exact_cols(kappa, x_ref, y_ref, fx_ref, s_ref, top_ref, weight_ref):
    cols = y_ref.shape[0]
    top_ref[...] = jnp.full(top_ref.shape, -jnp.inf, f32)
    weight_ref[...] = jnp.zeros(weight_ref.shape, f32)

    def chunk(c, carry):
        at = pl.multiple_of(c * LANES, LANES)
        z = cross_of(y_ref[...], x_ref[pl.ds(at, LANES), :]) * (2.0 * kappa) + fx_ref[pl.ds(c, 1), :]
        top = top_ref[...]
        newtop = jnp.maximum(top, jnp.max(z, axis=1, keepdims=True))
        weight_ref[...] = weight_ref[...] * jnp.exp2(top - newtop) + jnp.sum(
            jnp.exp2(z - newtop), axis=1, keepdims=True
        )
        top_ref[...] = newtop
        return carry

    lax.fori_loop(0, x_ref.shape[0] // LANES, chunk, 0)
    lse = top_ref[...] + log2(weight_ref[...]) - scaled_norms(y_ref[...], kappa)
    lane, sub = lane_and_sublane()
    for t in range(cols // LANES):
        line = jnp.zeros((8, LANES), f32)
        for q in range(LANES // 8):
            at = t * LANES + 8 * q
            line = line + jnp.where(lane == sub + 8 * q, lse[at : at + 8, :], 0.0)
        s_ref[t : t + 1, :] = jnp.sum(line, axis=0, keepdims=True)


def col_kernel(
    kappa, index, last,
    recv_ref, rm_ref, fprev_ref, mr_ref, xs_ref, sc_ref, errs_ref, k_ref, x_ref, y_ref,
    f_ref, sc_out_ref, errs_out_ref, out_ref,
    ubc_ref, acc_ref, s_ref, fx_ref, top_ref, weight_ref,
):
    rows, cols = k_ref.shape[1], k_ref.shape[0]
    lines = rows // LANES
    lane, sub = lane_and_sublane()
    lse = joined([recv_ref[d, 0:lines, :] for d in range(recv_ref.shape[0])])
    mass = rm_ref[...]
    la = log2(mass)
    sc = sc_ref[...]
    errs = errs_ref[...]
    if index == 0:
        f_new = la - lse
        mass_b = total(jnp.sum(recv_ref[:, lines : lines + 1, :], axis=0))
        sc = jnp.where(sub == 1, mass_b, 0.0)
        u = f_new + mr_ref[...]
        newest = largest(u)
        high = newest
    else:
        mass_a = sc[0:1, :]
        shift = log2(mass_a)
        f_new = la - shift - lse
        u = f_new + mr_ref[...]
        high = sc[2:3, :]
        f_old = fprev_ref[...]
        share = mass / mass_a
        if index == 1:
            errs = noted(errs, 0, jnp.abs(jnp.exp2(la - f_old) - share))
            f_old = f_old - shift
            high = high - shift
        errs = noted(errs, index, jnp.abs(jnp.exp2(la - shift + (f_old - f_new)) - share))
        newest = largest(u)
    weights = jnp.exp2(u - high)
    for l in range(lines):
        ubc_ref[:, l * LANES : (l + 1) * LANES] = jnp.broadcast_to(weights[l : l + 1, :], (8, LANES))
    together = 8

    def group(t, carry):
        acc = [None] * together
        lines_at = [pl.ds(pl.multiple_of((t * together + q) * 8, 8), 8) for q in range(together)]
        for l in range(lines):
            across = slice(l * LANES, (l + 1) * LANES)
            ul = ubc_ref[:, across]
            for q in range(together):
                term = k_ref[lines_at[q], across] * ul
                acc[q] = term if acc[q] is None else acc[q] + term
        for q in range(together):
            acc_ref[lines_at[q], :] = acc[q]
        return carry

    lax.fori_loop(0, cols // (8 * together), group, 0)
    for t in range(cols // LANES):
        picked = []
        for q in range(LANES // 8):
            at = t * LANES + 8 * q
            full = jnp.sum(acc_ref[at : at + 8, :], axis=1, keepdims=True)
            picked.append(jnp.where(lane == sub + 8 * q, full, 0.0))
        s_ref[t : t + 1, :] = jnp.sum(in_pairs(picked, jnp.add), axis=0, keepdims=True)
    sums = s_ref[...]
    extra = None
    if index == 0:
        extra = jnp.broadcast_to(jnp.sum(mass, axis=0, keepdims=True), (4, LANES))
    elif last:
        extra = jnp.broadcast_to(along_lanes(errs), (4, LANES))
    spread(out_ref, high + log2(sums), extra)
    f_ref[...] = f_new * (eps / LOG2E) if last else f_new
    sc_out_ref[...] = jnp.where(sub == 2, newest, sc)
    errs_out_ref[...] = errs
    least = jnp.min(jnp.where(newest - high <= DRIFT, sums, 0.0))

    @pl.when(jnp.logical_not(least >= SMALLEST))
    def _():
        fx_ref[...] = f_new - xs_ref[...]
        exact_cols(kappa, x_ref, y_ref, fx_ref, s_ref, top_ref, weight_ref)
        spread(out_ref, s_ref[...], extra)


def new_target(index, recv_ref, cm_ref, gprev_ref, sc, errs_ref):
    lines = cm_ref.shape[0]
    lane, sub = lane_and_sublane()
    lse = joined([recv_ref[d, 0:lines, :] for d in range(recv_ref.shape[0])])
    mass_b = sc[1:2, :]
    if index == 0:
        mass_a = total(jnp.sum(recv_ref[:, lines : lines + 1, :], axis=0))
        lse = lse - log2(mass_a)
        sc = jnp.where(sub == 0, mass_a, sc)
    mass = cm_ref[...]
    lb = log2(mass) - log2(mass_b)
    g_new = lb - lse
    errs = noted(errs_ref[...], index, jnp.abs(jnp.exp2(lb + (gprev_ref[...] - g_new)) - mass / mass_b))
    return g_new, sc, errs


def row_kernel(
    kappa, index,
    recv_ref, cm_ref, gprev_ref, mr_ref, xs_ref, sc_ref, errs_ref, k_ref, x_ref, y_ref,
    g_ref, sc_out_ref, errs_out_ref, out_ref,
    vbc_ref, r_ref, l_ref,
):
    rows, cols = k_ref.shape[1], k_ref.shape[0]
    lines = rows // LANES
    lane, sub = lane_and_sublane()
    sc = sc_ref[...]
    g_new, sc, errs = new_target(index, recv_ref, cm_ref, gprev_ref, sc, errs_ref)
    newest = largest(g_new)
    high = newest if index == 0 else sc[3:4, :]

    def put(at, piece):
        vbc_ref[at : at + 8, :] = piece

    column_form(jnp.exp2(g_new - high), put)
    together, block = min(16, lines), 32

    for first in range(0, lines, together):

        def group(b, acc, first=first):
            acc = list(acc)
            for j in range(block // 8):
                line = pl.ds(pl.multiple_of(b * block + 8 * j, 8), 8)
                vj = vbc_ref[line, :]
                for t in range(together):
                    across = slice((first + t) * LANES, (first + t + 1) * LANES)
                    acc[t] = acc[t] + k_ref[line, across] * vj
            return tuple(acc)

        acc = lax.fori_loop(0, cols // block, group, (jnp.zeros((8, LANES), f32),) * together)
        for t in range(together):
            r_ref[first + t : first + t + 1, :] = jnp.sum(acc[t], axis=0, keepdims=True)
    sums = r_ref[...]
    spread(out_ref, mr_ref[...] + (high + log2(sums)), None)
    g_ref[...] = g_new
    sc_out_ref[...] = jnp.where(sub == 3, newest, sc)
    errs_out_ref[...] = errs
    least = jnp.min(jnp.where(newest - high <= DRIFT, sums, 0.0))

    @pl.when(jnp.logical_not(least >= SMALLEST))
    def _():
        column_form(g_new, put)
        exact_rows(kappa, x_ref, y_ref, vbc_ref, xs_ref, l_ref)
        spread(out_ref, l_ref[...], None)


def last_kernel(index, recv_ref, cm_ref, gprev_ref, sc_ref, errs_ref, g_ref, row_ref, out_ref):
    lines = cm_ref.shape[0]
    g_new, sc, errs = new_target(index, recv_ref, cm_ref, gprev_ref, sc_ref[...], errs_ref)
    g_ref[...] = g_new * (eps / LOG2E)
    row_ref[...] = jnp.broadcast_to(jnp.sum(recv_ref[:, lines : lines + 1, :], axis=0), (8, LANES))
    col_errs = jnp.broadcast_to(along_lanes(errs), (8, LANES))
    for d in range(out_ref.shape[0]):
        out_ref[d] = col_errs


def on_chip():
    return pl.BlockSpec(memory_space=pltpu.VMEM)


def call(kernel, args, outs, scratch, limit, name):
    return pl.pallas_call(
        kernel,
        in_specs=[on_chip() for _ in args],
        out_specs=[on_chip() for _ in outs],
        out_shape=[jax.ShapeDtypeStruct(shape, f32) for shape in outs],
        scratch_shapes=[pltpu.VMEM(shape, f32) for shape in scratch],
        compiler_params=pltpu.CompilerParams(vmem_limit_bytes=limit),
        name=name,
    )(*args)


def exchange(x, axis):
    return lax.all_to_all(x, axis, split_axis=0, concat_axis=0, tiled=True)


def on_device(row_embed, col_embed, row_mass, col_mass):
    rows, width = row_embed.shape
    cols = col_embed.shape[0]
    kappa = LOG2E / (width * eps)
    row_lines, col_lines = rows // LANES, cols // LANES
    by_col = lax.axis_size(COLS_OVER)
    by_row = lax.axis_size(ROWS_OVER)
    rm = row_mass.reshape(row_lines, LANES)
    cm = col_mass.reshape(col_lines, LANES)
    tile = (8, LANES)
    mib = 1 << 20
    given = (row_embed, col_embed, rm, cm)
    blocks = [(cols, rows), (row_lines, LANES), (row_lines, LANES), (by_col, row_lines + 8, LANES)]
    row_embed, col_embed, rm, cm, k, mr, xs, out = pl.pallas_call(
        functools.partial(init_kernel, kappa),
        in_specs=[pl.BlockSpec(memory_space=pl.ANY) for _ in given],
        out_specs=[on_chip() for _ in range(len(given) + len(blocks))],
        out_shape=[jax.ShapeDtypeStruct(x.shape, x.dtype) for x in given]
        + [jax.ShapeDtypeStruct(shape, f32) for shape in blocks],
        scratch_shapes=[
            pltpu.VMEM((cols, LANES), f32),
            pltpu.VMEM((row_lines, LANES), f32),
            pltpu.SemaphoreType.DMA((len(given),)),
        ],
        compiler_params=pltpu.CompilerParams(vmem_limit_bytes=24 * mib),
        name="init",
    )(*given)
    f_pot = jnp.zeros((row_lines, LANES), f32)
    g_pot = jnp.zeros((col_lines, LANES), f32)
    sc = jnp.zeros(tile, f32)
    noting = (16, LANES)
    row_errs = jnp.zeros(noting, f32)
    col_errs = jnp.zeros(noting, f32)
    for index in range(ITERS):
        last = index == ITERS - 1
        got = exchange(out, COLS_OVER)
        more = 4 if index == 0 or last else 0
        f_pot, sc, row_errs, out = call(
            functools.partial(col_kernel, kappa, index, last),
            (got, rm, f_pot, mr, xs, sc, row_errs, k, row_embed, col_embed),
            [(row_lines, LANES), tile, noting, (by_row, col_lines + more, LANES)],
            [(8, rows), (cols, LANES), (col_lines, LANES), (row_lines, LANES), (cols, LANES), (cols, LANES)],
            24 * mib, f"cols{index}",
        )
        got = exchange(out, ROWS_OVER)
        if last:
            break
        g_pot, sc, col_errs, out = call(
            functools.partial(row_kernel, kappa, index),
            (got, cm, g_pot, mr, xs, sc, col_errs, k, row_embed, col_embed),
            [(col_lines, LANES), tile, noting, (by_col, row_lines, LANES)],
            [(cols, LANES), (row_lines, LANES), (row_lines, LANES)],
            24 * mib, f"rows{index}",
        )
    g_out, row_errs, out = call(
        functools.partial(last_kernel, ITERS - 1),
        (got, cm, g_pot, sc, col_errs),
        [(col_lines, LANES), tile, (by_col, 8, LANES)],
        [], 8 * mib, "finish",
    )
    got, row_errs = lax.optimization_barrier((exchange(out, COLS_OVER), row_errs))
    col_vec = jnp.sum(got[:, 0, :ITERS], axis=0)
    errors = jnp.stack([row_errs[0, :ITERS], col_vec], axis=1)
    return f_pot.reshape(rows), g_out.reshape(cols), errors


def solution(mesh):
    return jax.shard_map(
        on_device,
        mesh=mesh,
        in_specs=(P(ROWS_OVER, None), P(COLS_OVER, None), P(ROWS_OVER), P(COLS_OVER)),
        out_specs=(P(ROWS_OVER), P(COLS_OVER), P()),
        check_vma=False,
    )
```

```python
import functools
import math

import jax
import jax.numpy as jnp
from jax import lax
from jax.experimental import pallas as pl
from jax.experimental.pallas import tpu as pltpu
from jax.sharding import PartitionSpec as P

ITERS = 10
ROWS_OVER = ("gx", "gz")
COLS_OVER = "gy"
eps = 0.05
LOG2E = 1.0 / math.log(2.0)
LANES = 128
SMALLEST = 1e-20
DRIFT = 20.0
f32 = jnp.float32


def log2(x):
    return jnp.log(x) * LOG2E


def lane_and_sublane():
    return (
        lax.broadcasted_iota(jnp.int32, (8, LANES), 1),
        lax.broadcasted_iota(jnp.int32, (8, LANES), 0),
    )


def total(x):
    return jnp.sum(jnp.sum(x, axis=1, keepdims=True), axis=0, keepdims=True)


def largest(x):
    return jnp.max(jnp.max(x, axis=1, keepdims=True), axis=0, keepdims=True)


def scaled_norms(embed, kappa):
    wide = embed.astype(f32)
    return kappa * jnp.sum(wide * wide, axis=1, keepdims=True)


def cross_of(y, xb):
    return lax.dot_general(y, xb, (((1,), (1,)), ((), ())), preferred_element_type=f32)


def in_pairs(pieces, combine):
    while len(pieces) > 1:
        rest = [pieces[-1]] if len(pieces) % 2 else []
        pieces = [combine(*pair) for pair in zip(pieces[::2], pieces[1::2])] + rest
    return pieces[0]


def joined(pieces):
    top = in_pairs(pieces, jnp.maximum)
    return top + log2(in_pairs([jnp.exp2(piece - top) for piece in pieces], jnp.add))


def column_form(line, put):
    lane, sub = lane_and_sublane()
    for t in range(line.shape[0]):
        for q in range(LANES // 8):
            picked = jnp.where(lane == sub + 8 * q, line[t : t + 1, :], 0.0)
            put(t * LANES + 8 * q, jnp.broadcast_to(jnp.sum(picked, axis=1, keepdims=True), (8, LANES)))


def spread(out_ref, lines, extra):
    rows = lines.shape[0]
    for d in range(out_ref.shape[0]):
        out_ref[d, 0:rows, :] = lines
        if extra is not None:
            out_ref[d, rows : rows + extra.shape[0], :] = extra


def noted(errs, index, terms):
    row = lax.broadcasted_iota(jnp.int32, errs.shape, 0)
    return jnp.where(row == index, jnp.sum(terms, axis=0, keepdims=True), errs)


def along_lanes(errs):
    row = lax.broadcasted_iota(jnp.int32, errs.shape, 0)
    lane = lax.broadcasted_iota(jnp.int32, errs.shape, 1)
    picked = jnp.where(row == lane, jnp.sum(errs, axis=1, keepdims=True), 0.0)
    return jnp.sum(picked, axis=0, keepdims=True)


def init_kernel(kappa, x_ref, y_ref, cm_ref, k_ref, mr_ref, xs_ref, out_ref, cs_ref, l_ref):
    cols = y_ref.shape[0]
    rows = x_ref.shape[0]
    wide = 512
    cs_ref[...] = jnp.broadcast_to(scaled_norms(y_ref[...], kappa), (cols, LANES))
    ones = jnp.ones((8, x_ref.shape[1]), f32)

    def chunk(c, carry):
        at = pl.multiple_of(c * wide, wide)
        xb = x_ref[pl.ds(at, wide), :]
        k_ref[:, pl.ds(at, wide)] = cross_of(y_ref[...], xb) * (2.0 * kappa)
        xf = xb.astype(f32)
        norms = kappa * lax.dot_general(
            ones, xf * xf, (((1,), (1,)), ((), ())),
            precision=lax.Precision.HIGHEST, preferred_element_type=f32,
        )
        for t in range(wide // LANES):
            here = pl.ds(pl.multiple_of(at + t * LANES, LANES), LANES)
            tops = [None] * 4
            for j in range(cols // 8):
                z = k_ref[8 * j : 8 * j + 8, here] - cs_ref[8 * j : 8 * j + 8, :]
                tops[j % 4] = z if tops[j % 4] is None else jnp.maximum(tops[j % 4], z)
            top = jnp.maximum(jnp.maximum(tops[0], tops[1]), jnp.maximum(tops[2], tops[3]))
            top = jnp.max(top, axis=0, keepdims=True)
            sums = [None] * 4
            for j in range(cols // 8):
                e = jnp.exp2(k_ref[8 * j : 8 * j + 8, here] - cs_ref[8 * j : 8 * j + 8, :] - top)
                k_ref[8 * j : 8 * j + 8, here] = e
                sums[j % 4] = e if sums[j % 4] is None else sums[j % 4] + e
            weight = jnp.sum((sums[0] + sums[1]) + (sums[2] + sums[3]), axis=0, keepdims=True)
            norm = norms[0:1, t * LANES : (t + 1) * LANES]
            line = pl.ds(c * (wide // LANES) + t, 1)
            xs_ref[line, :] = norm
            mr_ref[line, :] = top - norm
            l_ref[line, :] = (top - norm) + log2(weight)
        return carry

    lax.fori_loop(0, rows // wide, chunk, 0)
    mass = jnp.broadcast_to(jnp.sum(cm_ref[...], axis=0, keepdims=True), (8, LANES))
    spread(out_ref, l_ref[...], mass)


def exact_rows(kappa, x_ref, y_ref, gcol_ref, xs_ref, l_ref):
    cols = y_ref.shape[0]
    cs = scaled_norms(y_ref[...], kappa)

    def chunk(c, carry):
        at = pl.multiple_of(c * LANES, LANES)
        z = cross_of(y_ref[...], x_ref[pl.ds(at, LANES), :]) * (2.0 * kappa) - cs + gcol_ref[...]
        top = jnp.max(z, axis=0, keepdims=True)
        weight = jnp.sum(jnp.exp2(z - top), axis=0, keepdims=True)
        l_ref[pl.ds(c, 1), :] = top - xs_ref[pl.ds(c, 1), :] + log2(weight)
        return carry

    lax.fori_loop(0, x_ref.shape[0] // LANES, chunk, 0)


def exact_cols(kappa, x_ref, y_ref, fx_ref, s_ref, top_ref, weight_ref):
    cols = y_ref.shape[0]
    top_ref[...] = jnp.full(top_ref.shape, -jnp.inf, f32)
    weight_ref[...] = jnp.zeros(weight_ref.shape, f32)

    def chunk(c, carry):
        at = pl.multiple_of(c * LANES, LANES)
        z = cross_of(y_ref[...], x_ref[pl.ds(at, LANES), :]) * (2.0 * kappa) + fx_ref[pl.ds(c, 1), :]
        top = top_ref[...]
        newtop = jnp.maximum(top, jnp.max(z, axis=1, keepdims=True))
        weight_ref[...] = weight_ref[...] * jnp.exp2(top - newtop) + jnp.sum(
            jnp.exp2(z - newtop), axis=1, keepdims=True
        )
        top_ref[...] = newtop
        return carry

    lax.fori_loop(0, x_ref.shape[0] // LANES, chunk, 0)
    lse = top_ref[...] + log2(weight_ref[...]) - scaled_norms(y_ref[...], kappa)
    lane, sub = lane_and_sublane()
    for t in range(cols // LANES):
        line = jnp.zeros((8, LANES), f32)
        for q in range(LANES // 8):
            at = t * LANES + 8 * q
            line = line + jnp.where(lane == sub + 8 * q, lse[at : at + 8, :], 0.0)
        s_ref[t : t + 1, :] = jnp.sum(line, axis=0, keepdims=True)


def col_kernel(
    kappa, index, last,
    recv_ref, rm_ref, fprev_ref, mr_ref, xs_ref, sc_ref, errs_ref, k_ref, x_ref, y_ref,
    f_ref, sc_out_ref, errs_out_ref, out_ref,
    acc_ref, s_ref, fx_ref, top_ref, weight_ref,
):
    rows, cols = k_ref.shape[1], k_ref.shape[0]
    lines = rows // LANES
    lane, sub = lane_and_sublane()
    lse = joined([recv_ref[d, 0:lines, :] for d in range(recv_ref.shape[0])])
    mass = rm_ref[...]
    la = log2(mass)
    sc = sc_ref[...]
    errs = errs_ref[...]
    if index == 0:
        f_new = la - lse
        mass_b = total(jnp.sum(recv_ref[:, lines : lines + 1, :], axis=0))
        sc = jnp.where(sub == 1, mass_b, 0.0)
        u = f_new + mr_ref[...]
        newest = largest(u)
        high = newest
    else:
        mass_a = sc[0:1, :]
        shift = log2(mass_a)
        f_new = la - shift - lse
        u = f_new + mr_ref[...]
        high = sc[2:3, :]
        f_old = fprev_ref[...]
        share = mass / mass_a
        if index == 1:
            errs = noted(errs, 0, jnp.abs(jnp.exp2(la - f_old) - share))
            f_old = f_old - shift
            high = high - shift
        errs = noted(errs, index, jnp.abs(jnp.exp2(la - shift + (f_old - f_new)) - share))
        newest = largest(u)
    weights = jnp.exp2(u - high)
    us = [jnp.broadcast_to(weights[l : l + 1, :], (8, LANES)) for l in range(lines)]
    together = 8

    def group(t, carry):
        acc = [None] * together
        lines_at = [pl.ds(pl.multiple_of((t * together + q) * 8, 8), 8) for q in range(together)]
        for q in range(together):
            parts = [None] * 2
            for l in range(lines):
                across = slice(l * LANES, (l + 1) * LANES)
                term = k_ref[lines_at[q], across] * us[l]
                parts[l % 2] = term if parts[l % 2] is None else parts[l % 2] + term
            acc[q] = parts[0] + parts[1]
        for q in range(together):
            acc_ref[lines_at[q], :] = acc[q]
        return carry

    lax.fori_loop(0, cols // (8 * together), group, 0)
    for t in range(cols // LANES):
        picked = []
        for q in range(LANES // 8):
            at = t * LANES + 8 * q
            full = jnp.sum(acc_ref[at : at + 8, :], axis=1, keepdims=True)
            picked.append(jnp.where(lane == sub + 8 * q, full, 0.0))
        s_ref[t : t + 1, :] = jnp.sum(in_pairs(picked, jnp.add), axis=0, keepdims=True)
    sums = s_ref[...]
    extra = None
    if index == 0:
        extra = jnp.broadcast_to(jnp.sum(mass, axis=0, keepdims=True), (4, LANES))
    elif last:
        extra = jnp.broadcast_to(along_lanes(errs), (4, LANES))
    spread(out_ref, high + log2(sums), extra)
    f_ref[...] = f_new * (eps / LOG2E) if last else f_new
    sc_out_ref[...] = jnp.where(sub == 2, newest, sc)
    errs_out_ref[...] = errs
    least = jnp.min(jnp.where(newest - high <= DRIFT, sums, 0.0))

    @pl.when(jnp.logical_not(least >= SMALLEST))
    def _():
        fx_ref[...] = f_new - xs_ref[...]
        exact_cols(kappa, x_ref, y_ref, fx_ref, s_ref, top_ref, weight_ref)
        spread(out_ref, s_ref[...], extra)


def new_target(index, recv_ref, cm_ref, gprev_ref, sc, errs_ref):
    lines = cm_ref.shape[0]
    lane, sub = lane_and_sublane()
    lse = joined([recv_ref[d, 0:lines, :] for d in range(recv_ref.shape[0])])
    mass_b = sc[1:2, :]
    if index == 0:
        mass_a = total(jnp.sum(recv_ref[:, lines : lines + 1, :], axis=0))
        lse = lse - log2(mass_a)
        sc = jnp.where(sub == 0, mass_a, sc)
    mass = cm_ref[...]
    lb = log2(mass) - log2(mass_b)
    g_new = lb - lse
    errs = noted(errs_ref[...], index, jnp.abs(jnp.exp2(lb + (gprev_ref[...] - g_new)) - mass / mass_b))
    return g_new, sc, errs


def row_kernel(
    kappa, index,
    recv_ref, cm_ref, gprev_ref, mr_ref, xs_ref, sc_ref, errs_ref, k_ref, x_ref, y_ref,
    g_ref, sc_out_ref, errs_out_ref, out_ref,
    vbc_ref, r_ref, l_ref,
):
    rows, cols = k_ref.shape[1], k_ref.shape[0]
    lines = rows // LANES
    lane, sub = lane_and_sublane()
    sc = sc_ref[...]
    g_new, sc, errs = new_target(index, recv_ref, cm_ref, gprev_ref, sc, errs_ref)
    newest = largest(g_new)
    high = newest if index == 0 else sc[3:4, :]

    def put(at, piece):
        vbc_ref[at : at + 8, :] = piece

    column_form(jnp.exp2(g_new - high), put)
    together, block = min(16, lines), 64

    for first in range(0, lines, together):

        def group(b, acc, first=first):
            acc = list(acc)
            for j in range(block // 8):
                line = pl.ds(pl.multiple_of(b * block + 8 * j, 8), 8)
                vj = vbc_ref[line, :]
                for t in range(together):
                    across = slice((first + t) * LANES, (first + t + 1) * LANES)
                    acc[t] = acc[t] + k_ref[line, across] * vj
            return tuple(acc)

        acc = lax.fori_loop(0, cols // block, group, (jnp.zeros((8, LANES), f32),) * together)
        for t in range(together):
            r_ref[first + t : first + t + 1, :] = jnp.sum(acc[t], axis=0, keepdims=True)
    sums = r_ref[...]
    spread(out_ref, mr_ref[...] + (high + log2(sums)), None)
    g_ref[...] = g_new
    sc_out_ref[...] = jnp.where(sub == 3, newest, sc)
    errs_out_ref[...] = errs
    least = jnp.min(jnp.where(newest - high <= DRIFT, sums, 0.0))

    @pl.when(jnp.logical_not(least >= SMALLEST))
    def _():
        column_form(g_new, put)
        exact_rows(kappa, x_ref, y_ref, vbc_ref, xs_ref, l_ref)
        spread(out_ref, l_ref[...], None)


def last_kernel(index, recv_ref, cm_ref, gprev_ref, sc_ref, errs_ref, g_ref, row_ref, out_ref):
    lines = cm_ref.shape[0]
    g_new, sc, errs = new_target(index, recv_ref, cm_ref, gprev_ref, sc_ref[...], errs_ref)
    g_ref[...] = g_new * (eps / LOG2E)
    row_ref[...] = jnp.broadcast_to(jnp.sum(recv_ref[:, lines : lines + 1, :], axis=0), (8, LANES))
    col_errs = jnp.broadcast_to(along_lanes(errs), (8, LANES))
    for d in range(out_ref.shape[0]):
        out_ref[d] = col_errs


def on_chip():
    return pl.BlockSpec(memory_space=pltpu.VMEM)


def call(kernel, args, outs, scratch, limit, name):
    return pl.pallas_call(
        kernel,
        in_specs=[on_chip() for _ in args],
        out_specs=[on_chip() for _ in outs],
        out_shape=[jax.ShapeDtypeStruct(shape, f32) for shape in outs],
        scratch_shapes=[pltpu.VMEM(shape, f32) for shape in scratch],
        compiler_params=pltpu.CompilerParams(vmem_limit_bytes=limit),
        name=name,
    )(*args)


def exchange(x, axis):
    return lax.all_to_all(x, axis, split_axis=0, concat_axis=0, tiled=True)


def on_device(row_embed, col_embed, row_mass, col_mass):
    rows, width = row_embed.shape
    cols = col_embed.shape[0]
    kappa = LOG2E / (width * eps)
    row_lines, col_lines = rows // LANES, cols // LANES
    by_col = lax.axis_size(COLS_OVER)
    by_row = lax.axis_size(ROWS_OVER)
    rm = row_mass.reshape(row_lines, LANES)
    cm = col_mass.reshape(col_lines, LANES)
    tile = (8, LANES)
    mib = 1 << 20
    k, mr, xs, out = call(
        functools.partial(init_kernel, kappa),
        (row_embed, col_embed, cm),
        [(cols, rows), (row_lines, LANES), (row_lines, LANES), (by_col, row_lines + 8, LANES)],
        [(cols, LANES), (row_lines, LANES)],
        24 * mib, "init",
    )
    f_pot = jnp.zeros((row_lines, LANES), f32)
    g_pot = jnp.zeros((col_lines, LANES), f32)
    sc = jnp.zeros(tile, f32)
    noting = (16, LANES)
    row_errs = jnp.zeros(noting, f32)
    col_errs = jnp.zeros(noting, f32)
    for index in range(ITERS):
        last = index == ITERS - 1
        got = exchange(out, COLS_OVER)
        more = 4 if index == 0 or last else 0
        f_pot, sc, row_errs, out = call(
            functools.partial(col_kernel, kappa, index, last),
            (got, rm, f_pot, mr, xs, sc, row_errs, k, row_embed, col_embed),
            [(row_lines, LANES), tile, noting, (by_row, col_lines + more, LANES)],
            [(cols, LANES), (col_lines, LANES), (row_lines, LANES), (cols, LANES), (cols, LANES)],
            24 * mib, f"cols{index}",
        )
        got = exchange(out, ROWS_OVER)
        if last:
            break
        g_pot, sc, col_errs, out = call(
            functools.partial(row_kernel, kappa, index),
            (got, cm, g_pot, mr, xs, sc, col_errs, k, row_embed, col_embed),
            [(col_lines, LANES), tile, noting, (by_col, row_lines, LANES)],
            [(cols, LANES), (row_lines, LANES), (row_lines, LANES)],
            24 * mib, f"rows{index}",
        )
    g_out, row_errs, out = call(
        functools.partial(last_kernel, ITERS - 1),
        (got, cm, g_pot, sc, col_errs),
        [(col_lines, LANES), tile, (by_col, 8, LANES)],
        [], 8 * mib, "finish",
    )
    got, row_errs = lax.optimization_barrier((exchange(out, COLS_OVER), row_errs))
    col_vec = jnp.sum(got[:, 0, :ITERS], axis=0)
    errors = jnp.stack([row_errs[0, :ITERS], col_vec], axis=1)
    return f_pot.reshape(rows), g_out.reshape(cols), errors


def solution(mesh):
    return jax.shard_map(
        on_device,
        mesh=mesh,
        in_specs=(P(ROWS_OVER, None), P(COLS_OVER, None), P(ROWS_OVER), P(COLS_OVER)),
        out_specs=(P(ROWS_OVER), P(COLS_OVER), P()),
        check_vma=False,
    )
```

```python
import functools
import math

import jax
import jax.numpy as jnp
from jax import lax
from jax.experimental import pallas as pl
from jax.experimental.pallas import tpu as pltpu
from jax.sharding import PartitionSpec as P

ITERS = 10
ROWS_OVER = ("gx", "gz")
COLS_OVER = "gy"
eps = 0.05
LOG2E = 1.0 / math.log(2.0)
LANES = 128
SMALLEST = 1e-20
DRIFT = 20.0
f32 = jnp.float32


def log2(x):
    return jnp.log(x) * LOG2E


def lane_and_sublane():
    return (
        lax.broadcasted_iota(jnp.int32, (8, LANES), 1),
        lax.broadcasted_iota(jnp.int32, (8, LANES), 0),
    )


def total(x):
    return jnp.sum(jnp.sum(x, axis=1, keepdims=True), axis=0, keepdims=True)


def largest(x):
    return jnp.max(jnp.max(x, axis=1, keepdims=True), axis=0, keepdims=True)


def scaled_norms(embed, kappa):
    wide = embed.astype(f32)
    return kappa * jnp.sum(wide * wide, axis=1, keepdims=True)


def cross_of(y, xb):
    return lax.dot_general(y, xb, (((1,), (1,)), ((), ())), preferred_element_type=f32)


def in_pairs(pieces, combine):
    while len(pieces) > 1:
        rest = [pieces[-1]] if len(pieces) % 2 else []
        pieces = [combine(*pair) for pair in zip(pieces[::2], pieces[1::2])] + rest
    return pieces[0]


def joined(pieces):
    top = in_pairs(pieces, jnp.maximum)
    return top + log2(in_pairs([jnp.exp2(piece - top) for piece in pieces], jnp.add))


def column_form(line, put):
    lane, sub = lane_and_sublane()
    for t in range(line.shape[0]):
        for q in range(LANES // 8):
            picked = jnp.where(lane == sub + 8 * q, line[t : t + 1, :], 0.0)
            put(t * LANES + 8 * q, jnp.broadcast_to(jnp.sum(picked, axis=1, keepdims=True), (8, LANES)))


def spread(out_ref, lines, extra):
    rows = lines.shape[0]
    for d in range(out_ref.shape[0]):
        out_ref[d, 0:rows, :] = lines
        if extra is not None:
            out_ref[d, rows : rows + extra.shape[0], :] = extra


def noted(errs, index, terms):
    row = lax.broadcasted_iota(jnp.int32, errs.shape, 0)
    return jnp.where(row == index, jnp.sum(terms, axis=0, keepdims=True), errs)


def along_lanes(errs):
    row = lax.broadcasted_iota(jnp.int32, errs.shape, 0)
    lane = lax.broadcasted_iota(jnp.int32, errs.shape, 1)
    picked = jnp.where(row == lane, jnp.sum(errs, axis=1, keepdims=True), 0.0)
    return jnp.sum(picked, axis=0, keepdims=True)


def init_kernel(kappa, x_ref, y_ref, cm_ref, k_ref, mr_ref, xs_ref, out_ref, cs_ref, l_ref):
    cols = y_ref.shape[0]
    rows = x_ref.shape[0]
    wide = 1024
    cs_ref[...] = jnp.broadcast_to(scaled_norms(y_ref[...], kappa), (cols, LANES))
    ones = jnp.ones((16, x_ref.shape[1]), jnp.bfloat16)

    def chunk(c, carry):
        at = pl.multiple_of(c * wide, wide)
        xb = x_ref[pl.ds(at, wide), :]
        kc_ref = k_ref.at[:, pl.ds(at, wide)]
        kc_ref[...] = cross_of(y_ref[...], xb) * (2.0 * kappa)
        squares = xb.astype(f32) * xb.astype(f32)
        upper = squares.astype(jnp.bfloat16)
        lower = (squares - upper.astype(f32)).astype(jnp.bfloat16)
        norms = kappa * (cross_of(ones, upper) + cross_of(ones, lower))
        tiles = wide // LANES
        here = [slice(t * LANES, (t + 1) * LANES) for t in range(tiles)]
        tops = [[None] * 2 for t in range(tiles)]
        for j in range(cols // 8):
            line = slice(8 * j, 8 * j + 8)
            cs = cs_ref[line, :]
            for t in range(tiles):
                z = kc_ref[line, here[t]] - cs
                tops[t][j % 2] = z if j < 2 else jnp.maximum(tops[t][j % 2], z)
        tops = [jnp.max(jnp.maximum(*pair), axis=0, keepdims=True) for pair in tops]
        spans = [jnp.broadcast_to(top, (8, LANES)) for top in tops]
        sums = [[None] * 2 for t in range(tiles)]
        for j in range(cols // 8):
            line = slice(8 * j, 8 * j + 8)
            cs = cs_ref[line, :]
            for t in range(tiles):
                e = jnp.exp2(kc_ref[line, here[t]] - cs - spans[t])
                kc_ref[line, here[t]] = e
                sums[t][j % 2] = e if j < 2 else sums[t][j % 2] + e
        for t in range(tiles):
            weight = jnp.sum(sums[t][0] + sums[t][1], axis=0, keepdims=True)
            norm = norms[0:1, t * LANES : (t + 1) * LANES]
            line = pl.ds(c * tiles + t, 1)
            xs_ref[line, :] = norm
            mr_ref[line, :] = tops[t] - norm
            l_ref[line, :] = (tops[t] - norm) + log2(weight)
        return carry

    lax.fori_loop(0, rows // wide, chunk, 0)
    mass = jnp.broadcast_to(jnp.sum(cm_ref[...], axis=0, keepdims=True), (8, LANES))
    spread(out_ref, l_ref[...], mass)


def exact_rows(kappa, x_ref, y_ref, gcol_ref, xs_ref, l_ref):
    cols = y_ref.shape[0]
    cs = scaled_norms(y_ref[...], kappa)

    def chunk(c, carry):
        at = pl.multiple_of(c * LANES, LANES)
        z = cross_of(y_ref[...], x_ref[pl.ds(at, LANES), :]) * (2.0 * kappa) - cs + gcol_ref[...]
        top = jnp.max(z, axis=0, keepdims=True)
        weight = jnp.sum(jnp.exp2(z - top), axis=0, keepdims=True)
        l_ref[pl.ds(c, 1), :] = top - xs_ref[pl.ds(c, 1), :] + log2(weight)
        return carry

    lax.fori_loop(0, x_ref.shape[0] // LANES, chunk, 0)


def exact_cols(kappa, x_ref, y_ref, fx_ref, s_ref, top_ref, weight_ref):
    cols = y_ref.shape[0]
    top_ref[...] = jnp.full(top_ref.shape, -jnp.inf, f32)
    weight_ref[...] = jnp.zeros(weight_ref.shape, f32)

    def chunk(c, carry):
        at = pl.multiple_of(c * LANES, LANES)
        z = cross_of(y_ref[...], x_ref[pl.ds(at, LANES), :]) * (2.0 * kappa) + fx_ref[pl.ds(c, 1), :]
        top = top_ref[...]
        newtop = jnp.maximum(top, jnp.max(z, axis=1, keepdims=True))
        weight_ref[...] = weight_ref[...] * jnp.exp2(top - newtop) + jnp.sum(
            jnp.exp2(z - newtop), axis=1, keepdims=True
        )
        top_ref[...] = newtop
        return carry

    lax.fori_loop(0, x_ref.shape[0] // LANES, chunk, 0)
    lse = top_ref[...] + log2(weight_ref[...]) - scaled_norms(y_ref[...], kappa)
    lane, sub = lane_and_sublane()
    for t in range(cols // LANES):
        line = jnp.zeros((8, LANES), f32)
        for q in range(LANES // 8):
            at = t * LANES + 8 * q
            line = line + jnp.where(lane == sub + 8 * q, lse[at : at + 8, :], 0.0)
        s_ref[t : t + 1, :] = jnp.sum(line, axis=0, keepdims=True)


def col_kernel(kappa, index, last, count, *refs):
    got, refs = refs[:count], refs[count:]
    rm_ref, fprev_ref, mr_ref, xs_ref, sc_ref, errs_ref, k_ref, x_ref, y_ref, *refs = refs
    f_ref, sc_out_ref, errs_out_ref, out_ref, *refs = refs
    acc_ref, s_ref, fx_ref, top_ref, weight_ref = refs
    rows, cols = k_ref.shape[1], k_ref.shape[0]
    lines = rows // LANES
    lane, sub = lane_and_sublane()
    if index == 0:
        recv_ref = got[0]
        lse = joined([recv_ref[d, 0:lines, :] for d in range(recv_ref.shape[0])])
    else:
        lse = joined([ref[...] for ref in got])
    mass = rm_ref[...]
    la = log2(mass)
    sc = sc_ref[...]
    errs = errs_ref[...]
    if index == 0:
        f_new = la - lse
        mass_b = total(jnp.sum(recv_ref[:, lines : lines + 1, :], axis=0))
        sc = jnp.where(sub == 1, mass_b, 0.0)
        u = f_new + mr_ref[...]
        newest = largest(u)
        high = newest
    else:
        mass_a = sc[0:1, :]
        shift = log2(mass_a)
        f_new = la - shift - lse
        u = f_new + mr_ref[...]
        high = sc[2:3, :]
        f_old = fprev_ref[...]
        share = mass / mass_a
        if index == 1:
            errs = noted(errs, 0, jnp.abs(jnp.exp2(la - f_old) - share))
            f_old = f_old - shift
            high = high - shift
        errs = noted(errs, index, jnp.abs(jnp.exp2(la - shift + (f_old - f_new)) - share))
        newest = largest(u)
    weights = jnp.exp2(u - high)
    us = [jnp.broadcast_to(weights[l : l + 1, :], (8, LANES)) for l in range(lines)]
    together = 8

    def group(t, carry):
        acc = [None] * together
        lines_at = [pl.ds(pl.multiple_of((t * together + q) * 8, 8), 8) for q in range(together)]
        for q in range(together):
            parts = [None] * 2
            for l in range(lines):
                across = slice(l * LANES, (l + 1) * LANES)
                term = k_ref[lines_at[q], across] * us[l]
                parts[l % 2] = term if parts[l % 2] is None else parts[l % 2] + term
            acc[q] = parts[0] + parts[1]
        for q in range(together):
            acc_ref[lines_at[q], :] = acc[q]
        return carry

    lax.fori_loop(0, cols // (8 * together), group, 0)
    for t in range(cols // LANES):
        picked = []
        for q in range(LANES // 8):
            at = t * LANES + 8 * q
            full = jnp.sum(acc_ref[at : at + 8, :], axis=1, keepdims=True)
            picked.append(jnp.where(lane == sub + 8 * q, full, 0.0))
        s_ref[t : t + 1, :] = jnp.sum(in_pairs(picked, jnp.add), axis=0, keepdims=True)
    sums = s_ref[...]
    extra = None
    if index == 0:
        extra = jnp.broadcast_to(jnp.sum(mass, axis=0, keepdims=True), (4, LANES))
    elif last:
        extra = jnp.broadcast_to(along_lanes(errs), (4, LANES))
    spread(out_ref, high + log2(sums), extra)
    f_ref[...] = f_new * (eps / LOG2E) if last else f_new
    sc_out_ref[...] = jnp.where(sub == 2, newest, sc)
    errs_out_ref[...] = errs
    least = jnp.min(jnp.where(newest - high <= DRIFT, sums, 0.0))

    @pl.when(jnp.logical_not(least >= SMALLEST))
    def _():
        fx_ref[...] = f_new - xs_ref[...]
        exact_cols(kappa, x_ref, y_ref, fx_ref, s_ref, top_ref, weight_ref)
        spread(out_ref, s_ref[...], extra)


def new_target(index, recv_ref, cm_ref, gprev_ref, sc, errs_ref):
    lines = cm_ref.shape[0]
    lane, sub = lane_and_sublane()
    lse = joined([recv_ref[d, 0:lines, :] for d in range(recv_ref.shape[0])])
    mass_b = sc[1:2, :]
    if index == 0:
        mass_a = total(jnp.sum(recv_ref[:, lines : lines + 1, :], axis=0))
        lse = lse - log2(mass_a)
        sc = jnp.where(sub == 0, mass_a, sc)
    mass = cm_ref[...]
    lb = log2(mass) - log2(mass_b)
    g_new = lb - lse
    errs = noted(errs_ref[...], index, jnp.abs(jnp.exp2(lb + (gprev_ref[...] - g_new)) - mass / mass_b))
    return g_new, sc, errs


def row_kernel(
    kappa, index,
    recv_ref, cm_ref, gprev_ref, mr_ref, xs_ref, sc_ref, errs_ref, k_ref, x_ref, y_ref,
    g_ref, sc_out_ref, errs_out_ref, out_ref,
    vbc_ref, r_ref, l_ref,
):
    rows, cols = k_ref.shape[1], k_ref.shape[0]
    lines = rows // LANES
    lane, sub = lane_and_sublane()
    sc = sc_ref[...]
    g_new, sc, errs = new_target(index, recv_ref, cm_ref, gprev_ref, sc, errs_ref)
    newest = largest(g_new)
    high = newest if index == 0 else sc[3:4, :]

    def put(at, piece):
        vbc_ref[at : at + 8, :] = piece

    column_form(jnp.exp2(g_new - high), put)
    together, block = min(16, lines), 64

    for first in range(0, lines, together):

        def group(b, acc, first=first):
            acc = list(acc)
            for j in range(block // 8):
                line = pl.ds(pl.multiple_of(b * block + 8 * j, 8), 8)
                vj = vbc_ref[line, :]
                for t in range(together):
                    across = slice((first + t) * LANES, (first + t + 1) * LANES)
                    acc[t] = acc[t] + k_ref[line, across] * vj
            return tuple(acc)

        acc = lax.fori_loop(0, cols // block, group, (jnp.zeros((8, LANES), f32),) * together)
        for t in range(together):
            r_ref[first + t : first + t + 1, :] = jnp.sum(acc[t], axis=0, keepdims=True)
    sums = r_ref[...]
    out_ref[...] = mr_ref[...] + (high + log2(sums))
    g_ref[...] = g_new
    sc_out_ref[...] = jnp.where(sub == 3, newest, sc)
    errs_out_ref[...] = errs
    least = jnp.min(jnp.where(newest - high <= DRIFT, sums, 0.0))

    @pl.when(jnp.logical_not(least >= SMALLEST))
    def _():
        column_form(g_new, put)
        exact_rows(kappa, x_ref, y_ref, vbc_ref, xs_ref, l_ref)
        out_ref[...] = l_ref[...]


def last_kernel(index, recv_ref, cm_ref, gprev_ref, sc_ref, errs_ref, g_ref, row_ref, out_ref):
    lines = cm_ref.shape[0]
    g_new, sc, errs = new_target(index, recv_ref, cm_ref, gprev_ref, sc_ref[...], errs_ref)
    g_ref[...] = g_new * (eps / LOG2E)
    row_ref[...] = jnp.broadcast_to(jnp.sum(recv_ref[:, lines : lines + 1, :], axis=0), (8, LANES))
    col_errs = jnp.broadcast_to(along_lanes(errs), (8, LANES))
    for d in range(out_ref.shape[0]):
        out_ref[d] = col_errs


def on_chip():
    return pl.BlockSpec(memory_space=pltpu.VMEM)


def call(kernel, args, outs, scratch, limit, name):
    return pl.pallas_call(
        kernel,
        in_specs=[on_chip() for _ in args],
        out_specs=[on_chip() for _ in outs],
        out_shape=[jax.ShapeDtypeStruct(shape, f32) for shape in outs],
        scratch_shapes=[pltpu.VMEM(shape, f32) for shape in scratch],
        compiler_params=pltpu.CompilerParams(vmem_limit_bytes=limit),
        name=name,
    )(*args)


def exchange(x, axis):
    return lax.all_to_all(x, axis, split_axis=0, concat_axis=0, tiled=True)


def paired(x, axis):
    count = lax.axis_size(axis)

    def swapped(x, by):
        return lax.ppermute(x, axis, [(i, i ^ by) for i in range(count)])

    both = joined([x, swapped(x, 1)])
    return (both, *(swapped(both, by) for by in range(2, count, 2)))


def on_device(row_embed, col_embed, row_mass, col_mass):
    rows, width = row_embed.shape
    cols = col_embed.shape[0]
    kappa = LOG2E / (width * eps)
    row_lines, col_lines = rows // LANES, cols // LANES
    by_col = lax.axis_size(COLS_OVER)
    by_row = lax.axis_size(ROWS_OVER)
    rm = row_mass.reshape(row_lines, LANES)
    cm = col_mass.reshape(col_lines, LANES)
    tile = (8, LANES)
    mib = 1 << 20
    k, mr, xs, out = call(
        functools.partial(init_kernel, kappa),
        (row_embed, col_embed, cm),
        [(cols, rows), (row_lines, LANES), (row_lines, LANES), (by_col, row_lines + 8, LANES)],
        [(cols, LANES), (row_lines, LANES)],
        24 * mib, "init",
    )
    f_pot = jnp.zeros((row_lines, LANES), f32)
    g_pot = jnp.zeros((col_lines, LANES), f32)
    sc = jnp.zeros(tile, f32)
    noting = (16, LANES)
    row_errs = jnp.zeros(noting, f32)
    col_errs = jnp.zeros(noting, f32)
    for index in range(ITERS):
        last = index == ITERS - 1
        got = (exchange(out, COLS_OVER),) if index == 0 else paired(out, COLS_OVER)
        more = 4 if index == 0 or last else 0
        f_pot, sc, row_errs, out = call(
            functools.partial(col_kernel, kappa, index, last, len(got)),
            (*got, rm, f_pot, mr, xs, sc, row_errs, k, row_embed, col_embed),
            [(row_lines, LANES), tile, noting, (by_row, col_lines + more, LANES)],
            [(cols, LANES), (col_lines, LANES), (row_lines, LANES), (cols, LANES), (cols, LANES)],
            24 * mib, f"cols{index}",
        )
        got = exchange(out, ROWS_OVER)
        if last:
            break
        g_pot, sc, col_errs, out = call(
            functools.partial(row_kernel, kappa, index),
            (got, cm, g_pot, mr, xs, sc, col_errs, k, row_embed, col_embed),
            [(col_lines, LANES), tile, noting, (row_lines, LANES)],
            [(cols, LANES), (row_lines, LANES), (row_lines, LANES)],
            24 * mib, f"rows{index}",
        )
    g_out, row_errs, out = call(
        functools.partial(last_kernel, ITERS - 1),
        (got, cm, g_pot, sc, col_errs),
        [(col_lines, LANES), tile, (by_col, 8, LANES)],
        [], 8 * mib, "finish",
    )
    got, row_errs = lax.optimization_barrier((exchange(out, COLS_OVER), row_errs))
    col_vec = jnp.sum(got[:, 0, :ITERS], axis=0)
    errors = jnp.stack([row_errs[0, :ITERS], col_vec], axis=1)
    return f_pot.reshape(rows), g_out.reshape(cols), errors


def solution(mesh):
    return jax.shard_map(
        on_device,
        mesh=mesh,
        in_specs=(P(ROWS_OVER, None), P(COLS_OVER, None), P(ROWS_OVER), P(COLS_OVER)),
        out_specs=(P(ROWS_OVER), P(COLS_OVER), P()),
        check_vma=False,
    )
```

```python
import functools
import math

import jax
import jax.numpy as jnp
from jax import lax
from jax.experimental import pallas as pl
from jax.experimental.pallas import tpu as pltpu
from jax.sharding import PartitionSpec as P


ITERS = 10
ROWS_OVER = ("gx", "gz")
COLS_OVER = "gy"
eps = 0.05
LOG2E = 1.0 / math.log(2.0)
LANES = 128
SMALLEST = 1e-20
DRIFT = 20.0
f32 = jnp.float32


def log2(x):
    return jnp.log(x) * LOG2E


def lane_and_sublane():
    return (
        lax.broadcasted_iota(jnp.int32, (8, LANES), 1),
        lax.broadcasted_iota(jnp.int32, (8, LANES), 0),
    )


def total(x):
    return jnp.sum(jnp.sum(x, axis=1, keepdims=True), axis=0, keepdims=True)


def largest(x):
    return jnp.max(jnp.max(x, axis=1, keepdims=True), axis=0, keepdims=True)


def scaled_norms(embed, kappa):
    wide = embed.astype(f32)
    return kappa * jnp.sum(wide * wide, axis=1, keepdims=True)


def cross_of(y, xb):
    return lax.dot_general(y, xb, (((1,), (1,)), ((), ())), preferred_element_type=f32)


def in_pairs(pieces, combine):
    while len(pieces) > 1:
        rest = [pieces[-1]] if len(pieces) % 2 else []
        pieces = [combine(*pair) for pair in zip(pieces[::2], pieces[1::2])] + rest
    return pieces[0]


def joined(pieces):
    top = in_pairs(pieces, jnp.maximum)
    return top + log2(in_pairs([jnp.exp2(piece - top) for piece in pieces], jnp.add))


def column_form(line, put):
    lane, sub = lane_and_sublane()
    for t in range(line.shape[0]):
        for q in range(LANES // 8):
            picked = jnp.where(lane == sub + 8 * q, line[t : t + 1, :], 0.0)
            put(t * LANES + 8 * q, jnp.broadcast_to(jnp.sum(picked, axis=1, keepdims=True), (8, LANES)))


def spread(out_ref, lines, extra):
    rows = lines.shape[0]
    for d in range(out_ref.shape[0]):
        out_ref[d, 0:rows, :] = lines
        if extra is not None:
            out_ref[d, rows : rows + extra.shape[0], :] = extra


def noted(errs, index, terms):
    row = lax.broadcasted_iota(jnp.int32, errs.shape, 0)
    return jnp.where(row == index, jnp.sum(terms, axis=0, keepdims=True), errs)


def along_lanes(errs):
    row = lax.broadcasted_iota(jnp.int32, errs.shape, 0)
    lane = lax.broadcasted_iota(jnp.int32, errs.shape, 1)
    picked = jnp.where(row == lane, jnp.sum(errs, axis=1, keepdims=True), 0.0)
    return jnp.sum(picked, axis=0, keepdims=True)


def init_kernel(kappa, x_ref, y_ref, cm_ref, k_ref, mr_ref, xs_ref, out_ref, cs_ref, l_ref):
    cols = y_ref.shape[0]
    rows = x_ref.shape[0]
    wide = 1024
    cs_ref[...] = jnp.broadcast_to(scaled_norms(y_ref[...], kappa), (cols, LANES))
    ones = jnp.ones((16, x_ref.shape[1]), jnp.bfloat16)

    def chunk(c, carry):
        at = pl.multiple_of(c * wide, wide)
        xb = x_ref[pl.ds(at, wide), :]
        kc_ref = k_ref.at[:, pl.ds(at, wide)]
        kc_ref[...] = cross_of(y_ref[...], xb) * (2.0 * kappa)
        squares = xb.astype(f32) * xb.astype(f32)
        upper = squares.astype(jnp.bfloat16)
        lower = (squares - upper.astype(f32)).astype(jnp.bfloat16)
        norms = kappa * (cross_of(ones, upper) + cross_of(ones, lower))
        tiles = wide // LANES
        here = [slice(t * LANES, (t + 1) * LANES) for t in range(tiles)]
        tops = [[None] * 2 for _ in range(tiles)]
        for j in range(cols // 8):
            line = slice(8 * j, 8 * j + 8)
            cs = cs_ref[line, :]
            for t in range(tiles):
                z = kc_ref[line, here[t]] - cs
                tops[t][j % 2] = z if j < 2 else jnp.maximum(tops[t][j % 2], z)
        tops = [jnp.max(jnp.maximum(*pair), axis=0, keepdims=True) for pair in tops]
        spans = [jnp.broadcast_to(top, (8, LANES)) for top in tops]
        sums = [[None] * 2 for _ in range(tiles)]
        for j in range(cols // 8):
            line = slice(8 * j, 8 * j + 8)
            cs = cs_ref[line, :]
            for t in range(tiles):
                e = jnp.exp2(kc_ref[line, here[t]] - cs - spans[t])
                kc_ref[line, here[t]] = e
                sums[t][j % 2] = e if j < 2 else sums[t][j % 2] + e
        for t in range(tiles):
            weight = jnp.sum(sums[t][0] + sums[t][1], axis=0, keepdims=True)
            norm = norms[0:1, t * LANES : (t + 1) * LANES]
            line = pl.ds(c * tiles + t, 1)
            xs_ref[line, :] = norm
            mr_ref[line, :] = tops[t] - norm
            l_ref[line, :] = (tops[t] - norm) + log2(weight)
        return carry

    lax.fori_loop(0, rows // wide, chunk, 0)
    mass = jnp.broadcast_to(jnp.sum(cm_ref[...], axis=0, keepdims=True), (8, LANES))
    spread(out_ref, l_ref[...], mass)


def exact_rows(kappa, x_ref, y_ref, gcol_ref, xs_ref, l_ref):
    def chunk(c, carry):
        xb = x_ref[pl.ds(pl.multiple_of(c * LANES, LANES), LANES), :]

        def part(b, kept):
            top, weight = kept
            here = pl.ds(pl.multiple_of(b * LANES, LANES), LANES)
            y = y_ref[here, :]
            z = cross_of(y, xb) * (2.0 * kappa) - scaled_norms(y, kappa) + gcol_ref[here, :]
            newtop = jnp.maximum(top, jnp.max(z, axis=0, keepdims=True))
            added = jnp.sum(jnp.exp2(z - newtop), axis=0, keepdims=True)
            return newtop, weight * jnp.exp2(top - newtop) + added

        nothing = (jnp.full((1, LANES), -jnp.inf, f32), jnp.zeros((1, LANES), f32))
        top, weight = lax.fori_loop(0, y_ref.shape[0] // LANES, part, nothing)
        l_ref[pl.ds(c, 1), :] = top - xs_ref[pl.ds(c, 1), :] + log2(weight)
        return carry

    lax.fori_loop(0, x_ref.shape[0] // LANES, chunk, 0)


def exact_cols(kappa, x_ref, y_ref, fx_ref, s_ref, top_ref, weight_ref):
    lane, sub = lane_and_sublane()

    def part(b, carry):
        y = y_ref[pl.ds(pl.multiple_of(b * LANES, LANES), LANES), :]
        top_ref[...] = jnp.full(top_ref.shape, -jnp.inf, f32)
        weight_ref[...] = jnp.zeros(weight_ref.shape, f32)

        def chunk(c, inner):
            xb = x_ref[pl.ds(pl.multiple_of(c * LANES, LANES), LANES), :]
            z = cross_of(y, xb) * (2.0 * kappa) + fx_ref[pl.ds(c, 1), :]
            top = top_ref[...]
            newtop = jnp.maximum(top, jnp.max(z, axis=1, keepdims=True))
            added = jnp.sum(jnp.exp2(z - newtop), axis=1, keepdims=True)
            weight_ref[...] = weight_ref[...] * jnp.exp2(top - newtop) + added
            top_ref[...] = newtop
            return inner

        lax.fori_loop(0, x_ref.shape[0] // LANES, chunk, 0)
        lse = top_ref[...] + log2(weight_ref[...]) - scaled_norms(y, kappa)
        line = jnp.zeros((8, LANES), f32)
        for q in range(LANES // 8):
            line = line + jnp.where(lane == sub + 8 * q, lse[8 * q : 8 * q + 8, :], 0.0)
        s_ref[pl.ds(b, 1), :] = jnp.sum(line, axis=0, keepdims=True)
        return carry

    lax.fori_loop(0, y_ref.shape[0] // LANES, part, 0)


def col_kernel(kappa, index, last, count, *refs):
    got, refs = refs[:count], refs[count:]
    rm_ref, fprev_ref, mr_ref, xs_ref, sc_ref, errs_ref, k_ref, x_ref, y_ref, *refs = refs
    f_ref, sc_out_ref, errs_out_ref, out_ref, *refs = refs
    acc_ref, s_ref, fx_ref, top_ref, weight_ref = refs
    rows, cols = k_ref.shape[1], k_ref.shape[0]
    lines = rows // LANES
    lane, sub = lane_and_sublane()
    if index == 0:
        recv_ref = got[0]
        lse = joined([recv_ref[d, 0:lines, :] for d in range(recv_ref.shape[0])])
    else:
        lse = joined([ref[...] for ref in got])
    mass = rm_ref[...]
    la = log2(mass)
    sc = sc_ref[...]
    errs = errs_ref[...]
    if index == 0:
        f_new = la - lse
        mass_b = total(jnp.sum(recv_ref[:, lines : lines + 1, :], axis=0))
        sc = jnp.where(sub == 1, mass_b, 0.0)
        u = f_new + mr_ref[...]
        newest = largest(u)
        high = newest
    else:
        mass_a = sc[0:1, :]
        shift = log2(mass_a)
        f_new = la - shift - lse
        u = f_new + mr_ref[...]
        high = sc[2:3, :]
        f_old = fprev_ref[...]
        share = mass / mass_a
        if index == 1:
            errs = noted(errs, 0, jnp.abs(jnp.exp2(la - f_old) - share))
            f_old = f_old - shift
            high = high - shift
        errs = noted(errs, index, jnp.abs(jnp.exp2(la - shift + (f_old - f_new)) - share))
        newest = largest(u)
    weights = jnp.exp2(u - high)
    us = [jnp.broadcast_to(weights[l : l + 1, :], (8, LANES)) for l in range(lines)]
    together = 8

    def group(t, carry):
        acc = [None] * together
        lines_at = [pl.ds(pl.multiple_of((t * together + q) * 8, 8), 8) for q in range(together)]
        for q in range(together):
            parts = [None] * 2
            for l in range(lines):
                across = slice(l * LANES, (l + 1) * LANES)
                term = k_ref[lines_at[q], across] * us[l]
                parts[l % 2] = term if parts[l % 2] is None else parts[l % 2] + term
            acc[q] = parts[0] + parts[1]
        for q in range(together):
            acc_ref[lines_at[q], :] = acc[q]
        return carry

    lax.fori_loop(0, cols // (8 * together), group, 0)
    for t in range(cols // LANES):
        picked = []
        for q in range(LANES // 8):
            at = t * LANES + 8 * q
            full = jnp.sum(acc_ref[at : at + 8, :], axis=1, keepdims=True)
            picked.append(jnp.where(lane == sub + 8 * q, full, 0.0))
        s_ref[t : t + 1, :] = jnp.sum(in_pairs(picked, jnp.add), axis=0, keepdims=True)
    sums = s_ref[...]
    extra = None
    if index == 0:
        extra = jnp.broadcast_to(jnp.sum(mass, axis=0, keepdims=True), (4, LANES))
    elif last:
        extra = jnp.broadcast_to(along_lanes(errs), (4, LANES))
    spread(out_ref, high + log2(sums), extra)
    f_ref[...] = f_new * (eps / LOG2E) if last else f_new
    sc_out_ref[...] = jnp.where(sub == 2, newest, sc)
    errs_out_ref[...] = errs
    least = jnp.min(jnp.where(newest - high <= DRIFT, sums, 0.0))

    @pl.when(jnp.logical_not(least >= SMALLEST))
    def _():
        fx_ref[...] = f_new - xs_ref[...]
        exact_cols(kappa, x_ref, y_ref, fx_ref, s_ref, top_ref, weight_ref)
        spread(out_ref, s_ref[...], extra)


def new_target(index, recv_ref, cm_ref, gprev_ref, sc, errs_ref):
    lines = cm_ref.shape[0]
    _, sub = lane_and_sublane()
    lse = joined([recv_ref[d, 0:lines, :] for d in range(recv_ref.shape[0])])
    mass_b = sc[1:2, :]
    if index == 0:
        mass_a = total(jnp.sum(recv_ref[:, lines : lines + 1, :], axis=0))
        lse = lse - log2(mass_a)
        sc = jnp.where(sub == 0, mass_a, sc)
    mass = cm_ref[...]
    lb = log2(mass) - log2(mass_b)
    g_new = lb - lse
    errs = noted(errs_ref[...], index, jnp.abs(jnp.exp2(lb + (gprev_ref[...] - g_new)) - mass / mass_b))
    return g_new, sc, errs


def row_kernel(
    kappa, index,
    recv_ref, cm_ref, gprev_ref, mr_ref, xs_ref, sc_ref, errs_ref, k_ref, x_ref, y_ref,
    g_ref, sc_out_ref, errs_out_ref, out_ref,
    vbc_ref, r_ref, l_ref,
):
    rows, cols = k_ref.shape[1], k_ref.shape[0]
    lines = rows // LANES
    _, sub = lane_and_sublane()
    sc = sc_ref[...]
    g_new, sc, errs = new_target(index, recv_ref, cm_ref, gprev_ref, sc, errs_ref)
    newest = largest(g_new)
    high = newest if index == 0 else sc[3:4, :]

    def put(at, piece):
        vbc_ref[at : at + 8, :] = piece

    column_form(jnp.exp2(g_new - high), put)
    together, block = min(16, lines), 64

    for first in range(0, lines, together):

        def group(b, acc, first=first):
            acc = list(acc)
            for j in range(block // 8):
                line = pl.ds(pl.multiple_of(b * block + 8 * j, 8), 8)
                vj = vbc_ref[line, :]
                for t in range(together):
                    across = slice((first + t) * LANES, (first + t + 1) * LANES)
                    acc[t] = acc[t] + k_ref[line, across] * vj
            return tuple(acc)

        acc = lax.fori_loop(0, cols // block, group, (jnp.zeros((8, LANES), f32),) * together)
        for t in range(together):
            r_ref[first + t : first + t + 1, :] = jnp.sum(acc[t], axis=0, keepdims=True)
    sums = r_ref[...]
    out_ref[...] = mr_ref[...] + (high + log2(sums))
    g_ref[...] = g_new
    sc_out_ref[...] = jnp.where(sub == 3, newest, sc)
    errs_out_ref[...] = errs
    least = jnp.min(jnp.where(newest - high <= DRIFT, sums, 0.0))

    @pl.when(jnp.logical_not(least >= SMALLEST))
    def _():
        column_form(g_new, put)
        exact_rows(kappa, x_ref, y_ref, vbc_ref, xs_ref, l_ref)
        out_ref[...] = l_ref[...]


def last_kernel(index, recv_ref, cm_ref, gprev_ref, sc_ref, errs_ref, g_ref, row_ref, out_ref):
    lines = cm_ref.shape[0]
    g_new, _, errs = new_target(index, recv_ref, cm_ref, gprev_ref, sc_ref[...], errs_ref)
    g_ref[...] = g_new * (eps / LOG2E)
    row_ref[...] = jnp.broadcast_to(jnp.sum(recv_ref[:, lines : lines + 1, :], axis=0), (8, LANES))
    col_errs = jnp.broadcast_to(along_lanes(errs), (8, LANES))
    for d in range(out_ref.shape[0]):
        out_ref[d] = col_errs


def on_chip():
    return pl.BlockSpec(memory_space=pltpu.VMEM)


def call(kernel, args, outs, scratch, limit):
    return pl.pallas_call(
        kernel,
        in_specs=[on_chip() for _ in args],
        out_specs=[on_chip() for _ in outs],
        out_shape=[jax.ShapeDtypeStruct(shape, f32) for shape in outs],
        scratch_shapes=[pltpu.VMEM(shape, f32) for shape in scratch],
        compiler_params=pltpu.CompilerParams(vmem_limit_bytes=limit),
    )(*args)


def exchange(x, axis):
    return lax.all_to_all(x, axis, split_axis=0, concat_axis=0, tiled=True)


def paired(x, axis):
    count = lax.axis_size(axis)

    def swapped(x, by):
        return lax.ppermute(x, axis, [(i, i ^ by) for i in range(count)])

    both = joined([x, swapped(x, 1)])
    return (both, *(swapped(both, by) for by in range(2, count, 2)))


def on_device(row_embed, col_embed, row_mass, col_mass):
    rows, width = row_embed.shape
    cols = col_embed.shape[0]
    kappa = LOG2E / (width * eps)
    row_lines, col_lines = rows // LANES, cols // LANES
    by_col = lax.axis_size(COLS_OVER)
    by_row = lax.axis_size(ROWS_OVER)
    rm = row_mass.reshape(row_lines, LANES)
    cm = col_mass.reshape(col_lines, LANES)
    tile = (8, LANES)
    mib = 1 << 20
    k, mr, xs, out = call(
        functools.partial(init_kernel, kappa),
        (row_embed, col_embed, cm),
        [(cols, rows), (row_lines, LANES), (row_lines, LANES), (by_col, row_lines + 8, LANES)],
        [(cols, LANES), (row_lines, LANES)],
        24 * mib,
    )
    f_pot = jnp.zeros((row_lines, LANES), f32)
    g_pot = jnp.zeros((col_lines, LANES), f32)
    sc = jnp.zeros(tile, f32)
    noting = (16, LANES)
    row_errs = jnp.zeros(noting, f32)
    col_errs = jnp.zeros(noting, f32)
    for index in range(ITERS):
        last = index == ITERS - 1
        got = (exchange(out, COLS_OVER),) if index == 0 else paired(out, COLS_OVER)
        more = 4 if index == 0 or last else 0
        f_pot, sc, row_errs, out = call(
            functools.partial(col_kernel, kappa, index, last, len(got)),
            (*got, rm, f_pot, mr, xs, sc, row_errs, k, row_embed, col_embed),
            [(row_lines, LANES), tile, noting, (by_row, col_lines + more, LANES)],
            [(cols, LANES), (col_lines, LANES), (row_lines, LANES), (LANES, LANES), (LANES, LANES)],
            24 * mib,
        )
        got = exchange(out, ROWS_OVER)
        if last:
            break
        g_pot, sc, col_errs, out = call(
            functools.partial(row_kernel, kappa, index),
            (got, cm, g_pot, mr, xs, sc, col_errs, k, row_embed, col_embed),
            [(col_lines, LANES), tile, noting, (row_lines, LANES)],
            [(cols, LANES), (row_lines, LANES), (row_lines, LANES)],
            24 * mib,
        )
    g_out, row_errs, out = call(
        functools.partial(last_kernel, ITERS - 1),
        (got, cm, g_pot, sc, col_errs),
        [(col_lines, LANES), tile, (by_col, 8, LANES)],
        [], 8 * mib,
    )
    got, row_errs = lax.optimization_barrier((exchange(out, COLS_OVER), row_errs))
    col_vec = jnp.sum(got[:, 0, :ITERS], axis=0)
    errors = jnp.stack([row_errs[0, :ITERS], col_vec], axis=1)
    return f_pot.reshape(rows), g_out.reshape(cols), errors


def solution(mesh):
    return jax.shard_map(
        on_device,
        mesh=mesh,
        in_specs=(P(ROWS_OVER, None), P(COLS_OVER, None), P(ROWS_OVER), P(COLS_OVER)),
        out_specs=(P(ROWS_OVER), P(COLS_OVER), P()),
        check_vma=False,
    )
```

```python
import functools
import math

import jax
import jax.numpy as jnp
from jax import lax
from jax.experimental import pallas as pl
from jax.experimental.pallas import tpu as pltpu
from jax.sharding import PartitionSpec as P

ITERS = 10
ROWS_OVER = ("gx", "gz")
COLS_OVER = "gy"
eps = 0.05
LOG2E = 1.0 / math.log(2.0)
LANES = 128
SMALLEST = 1e-20
DRIFT = 20.0
f32 = jnp.float32


def log2(x):
    return jnp.log(x) * LOG2E


def lane_and_sublane():
    return (
        lax.broadcasted_iota(jnp.int32, (8, LANES), 1),
        lax.broadcasted_iota(jnp.int32, (8, LANES), 0),
    )


def total(x):
    return jnp.sum(jnp.sum(x, axis=1, keepdims=True), axis=0, keepdims=True)


def largest(x):
    return jnp.max(jnp.max(x, axis=1, keepdims=True), axis=0, keepdims=True)


def scaled_norms(embed, kappa):
    wide = embed.astype(f32)
    return kappa * jnp.sum(wide * wide, axis=1, keepdims=True)


def cross_of(y, xb):
    return lax.dot_general(y, xb, (((1,), (1,)), ((), ())), preferred_element_type=f32)


def in_pairs(pieces, combine):
    while len(pieces) > 1:
        rest = [pieces[-1]] if len(pieces) % 2 else []
        pieces = [combine(*pair) for pair in zip(pieces[::2], pieces[1::2])] + rest
    return pieces[0]


def joined(pieces):
    top = in_pairs(pieces, jnp.maximum)
    return top + log2(in_pairs([jnp.exp2(piece - top) for piece in pieces], jnp.add))


def column_form(line, put):
    lane, sub = lane_and_sublane()
    for t in range(line.shape[0]):
        for q in range(LANES // 8):
            picked = jnp.where(lane == sub + 8 * q, line[t : t + 1, :], 0.0)
            put(t * LANES + 8 * q, jnp.broadcast_to(jnp.sum(picked, axis=1, keepdims=True), (8, LANES)))


def spread(out_ref, lines, extra):
    rows = lines.shape[0]
    for d in range(out_ref.shape[0]):
        out_ref[d, 0:rows, :] = lines
        if extra is not None:
            out_ref[d, rows : rows + extra.shape[0], :] = extra


def noted(errs, index, terms):
    row = lax.broadcasted_iota(jnp.int32, errs.shape, 0)
    return jnp.where(row == index, jnp.sum(terms, axis=0, keepdims=True), errs)


def along_lanes(errs):
    row = lax.broadcasted_iota(jnp.int32, errs.shape, 0)
    lane = lax.broadcasted_iota(jnp.int32, errs.shape, 1)
    picked = jnp.where(row == lane, jnp.sum(errs, axis=1, keepdims=True), 0.0)
    return jnp.sum(picked, axis=0, keepdims=True)


def init_kernel(kappa, x_ref, y_ref, cm_ref, k_ref, mr_ref, xs_ref, out_ref, cs_ref, l_ref):
    cols = y_ref.shape[0]
    rows = x_ref.shape[0]
    wide = 1024
    cs_ref[...] = jnp.broadcast_to(scaled_norms(y_ref[...], kappa), (cols, LANES))
    ones = jnp.ones((16, x_ref.shape[1]), jnp.bfloat16)

    def chunk(c, carry):
        at = pl.multiple_of(c * wide, wide)
        xb = x_ref[pl.ds(at, wide), :]
        kc_ref = k_ref.at[:, pl.ds(at, wide)]
        kc_ref[...] = cross_of(y_ref[...], xb) * (2.0 * kappa)
        squares = xb.astype(f32) * xb.astype(f32)
        upper = squares.astype(jnp.bfloat16)
        lower = (squares - upper.astype(f32)).astype(jnp.bfloat16)
        norms = kappa * (cross_of(ones, upper) + cross_of(ones, lower))
        tiles = wide // LANES
        here = [slice(t * LANES, (t + 1) * LANES) for t in range(tiles)]
        tops = [[None] * 2 for t in range(tiles)]
        for j in range(cols // 8):
            line = slice(8 * j, 8 * j + 8)
            cs = cs_ref[line, :]
            for t in range(tiles):
                z = kc_ref[line, here[t]] - cs
                tops[t][j % 2] = z if j < 2 else jnp.maximum(tops[t][j % 2], z)
        tops = [jnp.max(jnp.maximum(*pair), axis=0, keepdims=True) for pair in tops]
        spans = [jnp.broadcast_to(top, (8, LANES)) for top in tops]
        sums = [[None] * 2 for t in range(tiles)]
        for j in range(cols // 8):
            line = slice(8 * j, 8 * j + 8)
            cs = cs_ref[line, :]
            for t in range(tiles):
                e = jnp.exp2(kc_ref[line, here[t]] - cs - spans[t])
                kc_ref[line, here[t]] = e
                sums[t][j % 2] = e if j < 2 else sums[t][j % 2] + e
        for t in range(tiles):
            weight = jnp.sum(sums[t][0] + sums[t][1], axis=0, keepdims=True)
            norm = norms[0:1, t * LANES : (t + 1) * LANES]
            line = pl.ds(c * tiles + t, 1)
            xs_ref[line, :] = norm
            mr_ref[line, :] = tops[t] - norm
            l_ref[line, :] = (tops[t] - norm) + log2(weight)
        return carry

    lax.fori_loop(0, rows // wide, chunk, 0)
    mass = jnp.broadcast_to(jnp.sum(cm_ref[...], axis=0, keepdims=True), (8, LANES))
    spread(out_ref, l_ref[...], mass)


def widen_kernel(
    kappa, recv_ref, x_ref, other_ref, cm_ref, xs_ref, k_ref, mr_ref, y_ref, cmb_ref, cs_ref, base_ref
):
    cols, rows = k_ref.shape
    lines, col_lines = rows // LANES, cm_ref.shape[0]
    lse = joined([recv_ref[d, 0:lines, :] for d in range(recv_ref.shape[0])])
    mr_ref[...] = lse
    base_ref[...] = lse + xs_ref[...]
    y_ref[...] = other_ref[0:cols, :].astype(jnp.bfloat16)
    cs_ref[...] = jnp.broadcast_to(scaled_norms(other_ref[0:cols, :], kappa), (cols, LANES))
    cmb_ref[0:col_lines, :] = cm_ref[...]
    cmb_ref[col_lines : 2 * col_lines, :] = other_ref[cols : cols + col_lines, :]
    wide = 1024
    tiles = wide // LANES

    def chunk(c, carry):
        at = pl.multiple_of(c * wide, wide)
        kc_ref = k_ref.at[:, pl.ds(at, wide)]
        kc_ref[...] = cross_of(y_ref[...], x_ref[pl.ds(at, wide), :]) * (2.0 * kappa)
        spans = [jnp.broadcast_to(base_ref[pl.ds(c * tiles + t, 1), :], (8, LANES)) for t in range(tiles)]
        for j in range(cols // 8):
            line = slice(8 * j, 8 * j + 8)
            cs = cs_ref[line, :]
            for t in range(tiles):
                across = slice(t * LANES, (t + 1) * LANES)
                kc_ref[line, across] = jnp.exp2(kc_ref[line, across] - cs - spans[t])
        return carry

    lax.fori_loop(0, rows // wide, chunk, 0)


def exact_rows(kappa, x_ref, y_refs, gcol_ref, xs_ref, l_ref):
    def chunk(c, carry):
        xb = x_ref[pl.ds(pl.multiple_of(c * LANES, LANES), LANES), :]

        def part(b, kept, y_ref, first):
            top, weight = kept
            y = y_ref[pl.ds(pl.multiple_of(b * LANES, LANES), LANES), :]
            gain = gcol_ref[pl.ds(pl.multiple_of(first + b * LANES, LANES), LANES), :]
            z = cross_of(y, xb) * (2.0 * kappa) - scaled_norms(y, kappa) + gain
            newtop = jnp.maximum(top, jnp.max(z, axis=0, keepdims=True))
            added = jnp.sum(jnp.exp2(z - newtop), axis=0, keepdims=True)
            return newtop, weight * jnp.exp2(top - newtop) + added

        kept = (jnp.full((1, LANES), -jnp.inf, f32), jnp.zeros((1, LANES), f32))
        first = 0
        for y_ref in y_refs:
            one = functools.partial(part, y_ref=y_ref, first=first)
            kept = lax.fori_loop(0, y_ref.shape[0] // LANES, one, kept)
            first += y_ref.shape[0]
        top, weight = kept
        l_ref[pl.ds(c, 1), :] = top - xs_ref[pl.ds(c, 1), :] + log2(weight)
        return carry

    lax.fori_loop(0, x_ref.shape[0] // LANES, chunk, 0)


def exact_cols(kappa, x_ref, y_ref, first, fx_ref, s_ref, top_ref, weight_ref):
    lane, sub = lane_and_sublane()

    def part(b, carry):
        y = y_ref[pl.ds(pl.multiple_of(b * LANES, LANES), LANES), :]
        top_ref[...] = jnp.full(top_ref.shape, -jnp.inf, f32)
        weight_ref[...] = jnp.zeros(weight_ref.shape, f32)

        def chunk(c, inner):
            xb = x_ref[pl.ds(pl.multiple_of(c * LANES, LANES), LANES), :]
            z = cross_of(y, xb) * (2.0 * kappa) + fx_ref[pl.ds(c, 1), :]
            top = top_ref[...]
            newtop = jnp.maximum(top, jnp.max(z, axis=1, keepdims=True))
            added = jnp.sum(jnp.exp2(z - newtop), axis=1, keepdims=True)
            weight_ref[...] = weight_ref[...] * jnp.exp2(top - newtop) + added
            top_ref[...] = newtop
            return inner

        lax.fori_loop(0, x_ref.shape[0] // LANES, chunk, 0)
        lse = top_ref[...] + log2(weight_ref[...]) - scaled_norms(y, kappa)
        line = jnp.zeros((8, LANES), f32)
        for q in range(LANES // 8):
            line = line + jnp.where(lane == sub + 8 * q, lse[8 * q : 8 * q + 8, :], 0.0)
        s_ref[pl.ds(first + b, 1), :] = jnp.sum(line, axis=0, keepdims=True)
        return carry

    lax.fori_loop(0, y_ref.shape[0] // LANES, part, 0)


def col_kernel(kappa, index, last, count, *refs):
    got, refs = refs[:count], refs[count:]
    rm_ref, fprev_ref, mr_ref, mr2_ref, xs_ref, sc_ref, errs_ref, k_ref, k2_ref, x_ref, y_ref, y2_ref, *refs = refs
    f_ref, sc_out_ref, errs_out_ref, out_ref, *refs = refs
    acc_ref, s_ref, fx_ref, top_ref, weight_ref = refs
    rows, cols = k_ref.shape[1], k_ref.shape[0]
    lines = rows // LANES
    lane, sub = lane_and_sublane()
    if index == 0:
        recv_ref = got[0]
        lse = joined([recv_ref[d, 0:lines, :] for d in range(recv_ref.shape[0])])
    else:
        lse = joined([ref[...] for ref in got])
    mass = rm_ref[...]
    la = log2(mass)
    sc = sc_ref[...]
    errs = errs_ref[...]
    if index == 0:
        f_new = la - lse
        mass_b = total(jnp.sum(recv_ref[:, lines : lines + 1, :], axis=0))
        sc = jnp.where(sub == 1, mass_b, 0.0)
        u = [f_new + ref[...] for ref in (mr_ref, mr2_ref)]
        newest = [largest(part) for part in u]
        high = newest
    else:
        mass_a = sc[0:1, :]
        shift = log2(mass_a)
        f_new = la - shift - lse
        u = [f_new + ref[...] for ref in (mr_ref, mr2_ref)]
        high = [sc[2:3, :], sc[4:5, :]]
        f_old = fprev_ref[...]
        share = mass / mass_a
        if index == 1:
            errs = noted(errs, 0, jnp.abs(jnp.exp2(la - f_old) - share))
            f_old = f_old - shift
            high = [part - shift for part in high]
        errs = noted(errs, index, jnp.abs(jnp.exp2(la - shift + (f_old - f_new)) - share))
        newest = [largest(part) for part in u]
    together = 8
    for half, matrix in enumerate((k_ref, k2_ref)):
        weights = jnp.exp2(u[half] - high[half])
        us = [jnp.broadcast_to(weights[l : l + 1, :], (8, LANES)) for l in range(lines)]

        def group(t, carry, us=us, matrix=matrix, first=half * cols):
            for q in range(together):
                line = pl.ds(pl.multiple_of((t * together + q) * 8, 8), 8)
                parts = [None] * 2
                for l in range(lines):
                    term = matrix[line, l * LANES : (l + 1) * LANES] * us[l]
                    parts[l % 2] = term if parts[l % 2] is None else parts[l % 2] + term
                acc_ref[pl.ds(pl.multiple_of(first + (t * together + q) * 8, 8), 8), :] = parts[0] + parts[1]
            return carry

        lax.fori_loop(0, cols // (8 * together), group, 0)
    for t in range(2 * cols // LANES):
        picked = []
        for q in range(LANES // 8):
            at = t * LANES + 8 * q
            full = jnp.sum(acc_ref[at : at + 8, :], axis=1, keepdims=True)
            picked.append(jnp.where(lane == sub + 8 * q, full, 0.0))
        s_ref[t : t + 1, :] = jnp.sum(in_pairs(picked, jnp.add), axis=0, keepdims=True)
    sums = s_ref[...]
    extra = None
    if index == 0:
        extra = jnp.broadcast_to(jnp.sum(mass, axis=0, keepdims=True), (8, LANES))
    elif last:
        extra = jnp.broadcast_to(along_lanes(errs), (8, LANES))
    own = lax.broadcasted_iota(jnp.int32, sums.shape, 0) < cols // LANES
    spread(out_ref, jnp.where(own, high[0], high[1]) + log2(sums), extra)
    f_ref[...] = f_new * (eps / LOG2E) if last else f_new
    sc_out_ref[...] = jnp.where(sub == 2, newest[0], jnp.where(sub == 4, newest[1], sc))
    errs_out_ref[...] = errs
    drift = jnp.maximum(newest[0] - high[0], newest[1] - high[1])
    least = jnp.min(jnp.where(drift <= DRIFT, sums, 0.0))

    @pl.when(jnp.logical_not(least >= SMALLEST))
    def _():
        fx_ref[...] = f_new - xs_ref[...]
        exact_cols(kappa, x_ref, y_ref, 0, fx_ref, s_ref, top_ref, weight_ref)
        exact_cols(kappa, x_ref, y2_ref, cols // LANES, fx_ref, s_ref, top_ref, weight_ref)
        spread(out_ref, s_ref[...], extra)


def new_target(index, recv_ref, cm_ref, gprev_ref, sc, errs_ref):
    lines = cm_ref.shape[0]
    lane, sub = lane_and_sublane()
    lse = joined([recv_ref[d, 0:lines, :] for d in range(recv_ref.shape[0])])
    mass_b = sc[1:2, :]
    if index == 0:
        mass_a = total(jnp.sum(recv_ref[:, lines : lines + 1, :], axis=0))
        lse = lse - log2(mass_a)
        sc = jnp.where(sub == 0, mass_a, sc)
    mass = cm_ref[...]
    lb = log2(mass) - log2(mass_b)
    g_new = lb - lse
    terms = jnp.abs(jnp.exp2(lb + (gprev_ref[...] - g_new)) - mass / mass_b)
    errs = noted(errs_ref[...], index, terms[0 : lines // 2, :])
    return g_new, sc, errs


def row_kernel(
    kappa, index,
    recv_ref, cm_ref, gprev_ref, mr_ref, mr2_ref, xs_ref, sc_ref, errs_ref, k_ref, k2_ref, x_ref, y_ref, y2_ref,
    g_ref, sc_out_ref, errs_out_ref, out_ref,
    vbc_ref, r_ref, l_ref,
):
    rows, cols = k_ref.shape[1], k_ref.shape[0]
    lines = rows // LANES
    lane, sub = lane_and_sublane()
    sc = sc_ref[...]
    g_new, sc, errs = new_target(index, recv_ref, cm_ref, gprev_ref, sc, errs_ref)
    newest = largest(g_new)
    high = newest if index == 0 else sc[3:4, :]

    def put(at, piece):
        vbc_ref[at : at + 8, :] = piece

    column_form(jnp.exp2(g_new - high), put)
    together, block = min(16, lines), 64

    for half, matrix in enumerate((k_ref, k2_ref)):
        for first in range(0, lines, together):

            def group(b, acc, first=first, matrix=matrix, start=half * cols):
                acc = list(acc)
                for j in range(block // 8):
                    line = pl.ds(pl.multiple_of(b * block + 8 * j, 8), 8)
                    vj = vbc_ref[pl.ds(pl.multiple_of(start + b * block + 8 * j, 8), 8), :]
                    for t in range(together):
                        across = slice((first + t) * LANES, (first + t + 1) * LANES)
                        acc[t] = acc[t] + matrix[line, across] * vj
                return tuple(acc)

            acc = lax.fori_loop(0, cols // block, group, (jnp.zeros((8, LANES), f32),) * together)
            for t in range(together):
                at = half * lines + first + t
                r_ref[at : at + 1, :] = jnp.sum(acc[t], axis=0, keepdims=True)
    sums = [r_ref[0:lines, :], r_ref[lines : 2 * lines, :]]
    out_ref[...] = joined([ref[...] + (high + log2(part)) for ref, part in zip((mr_ref, mr2_ref), sums)])
    g_ref[...] = g_new
    sc_out_ref[...] = jnp.where(sub == 3, newest, sc)
    errs_out_ref[...] = errs
    least = jnp.min(jnp.where(newest - high <= DRIFT, jnp.minimum(*sums), 0.0))

    @pl.when(jnp.logical_not(least >= SMALLEST))
    def _():
        column_form(g_new, put)
        exact_rows(kappa, x_ref, (y_ref, y2_ref), vbc_ref, xs_ref, l_ref)
        out_ref[...] = l_ref[...]


def last_kernel(index, recv_ref, cm_ref, gprev_ref, sc_ref, errs_ref, g_ref, row_ref, out_ref):
    lines = cm_ref.shape[0]
    g_new, sc, errs = new_target(index, recv_ref, cm_ref, gprev_ref, sc_ref[...], errs_ref)
    g_ref[...] = g_new[0 : lines // 2, :] * (eps / LOG2E)
    row_ref[...] = jnp.broadcast_to(jnp.sum(recv_ref[:, lines : lines + 1, :], axis=0), (8, LANES))
    col_errs = jnp.broadcast_to(along_lanes(errs), (8, LANES))
    for d in range(out_ref.shape[0]):
        out_ref[d] = col_errs


def on_chip():
    return pl.BlockSpec(memory_space=pltpu.VMEM)


def call(kernel, args, outs, scratch, limit, name):
    return pl.pallas_call(
        kernel,
        in_specs=[on_chip() for _ in args],
        out_specs=[on_chip() for _ in outs],
        out_shape=[jax.ShapeDtypeStruct(shape, f32) for shape in outs],
        scratch_shapes=[pltpu.VMEM(shape, f32) for shape in scratch],
        compiler_params=pltpu.CompilerParams(vmem_limit_bytes=limit),
        name=name,
    )(*args)


def exchange(x, axis):
    return lax.all_to_all(x, axis, split_axis=0, concat_axis=0, tiled=True)


def swapped(x, by):
    count = lax.axis_size(COLS_OVER)
    return lax.ppermute(x, COLS_OVER, [(i, i ^ by) for i in range(count)])


def paired(x):
    both = joined([x, swapped(x, 1)])
    return (both, *(swapped(both, by) for by in range(2, lax.axis_size(COLS_OVER) // 2, 2)))


def on_device(row_embed, col_embed, row_mass, col_mass):
    rows, width = row_embed.shape
    cols = col_embed.shape[0]
    kappa = LOG2E / (width * eps)
    row_lines, col_lines = rows // LANES, cols // LANES
    by_col = lax.axis_size(COLS_OVER)
    by_row = lax.axis_size(ROWS_OVER)
    rm = row_mass.reshape(row_lines, LANES)
    cm = col_mass.reshape(col_lines, LANES)
    tile = (8, LANES)
    padding = jnp.zeros((-col_lines % 8, LANES), f32)
    other = swapped(jnp.concatenate([col_embed.astype(f32), cm, padding]), by_col // 2)
    mib = 1 << 20
    k, mr, xs, out = call(
        functools.partial(init_kernel, kappa),
        (row_embed, col_embed, cm),
        [(cols, rows), (row_lines, LANES), (row_lines, LANES), (by_col, row_lines + 8, LANES)],
        [(cols, LANES), (row_lines, LANES)],
        24 * mib, "init",
    )
    f_pot = jnp.zeros((row_lines, LANES), f32)
    g_pot = jnp.zeros((2 * col_lines, LANES), f32)
    sc = jnp.zeros(tile, f32)
    noting = (16, LANES)
    row_errs = jnp.zeros(noting, f32)
    col_errs = jnp.zeros(noting, f32)
    vmem = pltpu.VMEM
    for index in range(ITERS):
        last = index == ITERS - 1
        if index == 0:
            got = (exchange(out, COLS_OVER),)
            k2, mr2, y2, cmb = pl.pallas_call(
                functools.partial(widen_kernel, kappa),
                in_specs=[on_chip() for _ in range(5)],
                out_specs=[on_chip() for _ in range(4)],
                out_shape=[
                    jax.ShapeDtypeStruct((cols, rows), f32),
                    jax.ShapeDtypeStruct((row_lines, LANES), f32),
                    jax.ShapeDtypeStruct(col_embed.shape, col_embed.dtype),
                    jax.ShapeDtypeStruct((2 * col_lines, LANES), f32),
                ],
                scratch_shapes=[vmem((cols, LANES), f32), vmem((row_lines, LANES), f32)],
                compiler_params=pltpu.CompilerParams(vmem_limit_bytes=24 * mib),
                name="widen",
            )(got[0], row_embed, other, cm, xs)
        else:
            got = paired(out)
        more = 8 if index == 0 or last else 0
        fixed = (k, k2, row_embed, col_embed, y2)
        f_pot, sc, row_errs, out = call(
            functools.partial(col_kernel, kappa, index, last, len(got)),
            (*got, rm, f_pot, mr, mr2, xs, sc, row_errs, *fixed),
            [(row_lines, LANES), tile, noting, (by_row, 2 * col_lines + more, LANES)],
            [(2 * cols, LANES), (2 * col_lines, LANES), (row_lines, LANES), (LANES, LANES), (LANES, LANES)],
            24 * mib, f"cols{index}",
        )
        got = exchange(out, ROWS_OVER)
        if last:
            break
        g_pot, sc, col_errs, out = call(
            functools.partial(row_kernel, kappa, index),
            (got, cmb, g_pot, mr, mr2, xs, sc, col_errs, *fixed),
            [(2 * col_lines, LANES), tile, noting, (row_lines, LANES)],
            [(2 * cols, LANES), (2 * row_lines, LANES), (row_lines, LANES)],
            24 * mib, f"rows{index}",
        )
    g_out, row_errs, out = call(
        functools.partial(last_kernel, ITERS - 1),
        (got, cmb, g_pot, sc, col_errs),
        [(col_lines, LANES), tile, (by_col, 8, LANES)],
        [], 8 * mib, "finish",
    )
    got, row_errs = lax.optimization_barrier((exchange(out, COLS_OVER), row_errs))
    col_vec = jnp.sum(got[:, 0, :ITERS], axis=0)
    errors = jnp.stack([row_errs[0, :ITERS], col_vec], axis=1)
    return f_pot.reshape(rows), g_out.reshape(cols), errors


def solution(mesh):
    return jax.shard_map(
        on_device,
        mesh=mesh,
        in_specs=(P(ROWS_OVER, None), P(COLS_OVER, None), P(ROWS_OVER), P(COLS_OVER)),
        out_specs=(P(ROWS_OVER), P(COLS_OVER), P()),
        check_vma=False,
    )
```

```python
import functools
import math

import jax
import jax.numpy as jnp
from jax import lax
from jax.experimental import pallas as pl
from jax.experimental.pallas import tpu as pltpu
from jax.sharding import PartitionSpec as P

ITERS = 10
ROWS_OVER = ("gx", "gz")
COLS_OVER = "gy"
eps = 0.05
LOG2E = 1.0 / math.log(2.0)
LANES = 128
SMALLEST = 1e-20
DRIFT = 20.0
f32 = jnp.float32


def log2(x):
    return jnp.log(x) * LOG2E


def lane_and_sublane():
    return (
        lax.broadcasted_iota(jnp.int32, (8, LANES), 1),
        lax.broadcasted_iota(jnp.int32, (8, LANES), 0),
    )


def total(x):
    return jnp.sum(jnp.sum(x, axis=1, keepdims=True), axis=0, keepdims=True)


def largest(x):
    return jnp.max(jnp.max(x, axis=1, keepdims=True), axis=0, keepdims=True)


def scaled_norms(embed, kappa):
    wide = embed.astype(f32)
    return kappa * jnp.sum(wide * wide, axis=1, keepdims=True)


def cross_of(y, xb):
    return lax.dot_general(y, xb, (((1,), (1,)), ((), ())), preferred_element_type=f32)


def in_pairs(pieces, combine):
    while len(pieces) > 1:
        rest = [pieces[-1]] if len(pieces) % 2 else []
        pieces = [combine(*pair) for pair in zip(pieces[::2], pieces[1::2])] + rest
    return pieces[0]


def joined(pieces):
    top = in_pairs(pieces, jnp.maximum)
    return top + log2(in_pairs([jnp.exp2(piece - top) for piece in pieces], jnp.add))


def column_form(line, put):
    lane, sub = lane_and_sublane()
    for t in range(line.shape[0]):
        for q in range(LANES // 8):
            picked = jnp.where(lane == sub + 8 * q, line[t : t + 1, :], 0.0)
            put(t * LANES + 8 * q, jnp.broadcast_to(jnp.sum(picked, axis=1, keepdims=True), (8, LANES)))


def spread(out_ref, lines, extra):
    rows = lines.shape[0]
    for d in range(out_ref.shape[0]):
        out_ref[d, 0:rows, :] = lines
        if extra is not None:
            out_ref[d, rows : rows + extra.shape[0], :] = extra


def noted(errs, index, terms):
    row = lax.broadcasted_iota(jnp.int32, errs.shape, 0)
    return jnp.where(row == index, jnp.sum(terms, axis=0, keepdims=True), errs)


def along_lanes(errs):
    row = lax.broadcasted_iota(jnp.int32, errs.shape, 0)
    lane = lax.broadcasted_iota(jnp.int32, errs.shape, 1)
    picked = jnp.where(row == lane, jnp.sum(errs, axis=1, keepdims=True), 0.0)
    return jnp.sum(picked, axis=0, keepdims=True)


def init_kernel(kappa, x_ref, y_ref, cm_ref, k_ref, mr_ref, xs_ref, out_ref, own_ref, pack_ref, cs_ref, l_ref):
    cols = y_ref.shape[0]
    rows = x_ref.shape[0]
    wide = 1024
    cs_ref[...] = jnp.broadcast_to(scaled_norms(y_ref[...], kappa), (cols, LANES))
    ones = jnp.ones((16, x_ref.shape[1]), jnp.bfloat16)

    def chunk(c, carry):
        at = pl.multiple_of(c * wide, wide)
        xb = x_ref[pl.ds(at, wide), :]
        kc_ref = k_ref.at[:, pl.ds(at, wide)]
        kc_ref[...] = cross_of(y_ref[...], xb) * (2.0 * kappa)
        squares = xb.astype(f32) * xb.astype(f32)
        upper = squares.astype(jnp.bfloat16)
        lower = (squares - upper.astype(f32)).astype(jnp.bfloat16)
        norms = kappa * (cross_of(ones, upper) + cross_of(ones, lower))
        tiles = wide // LANES
        here = [slice(t * LANES, (t + 1) * LANES) for t in range(tiles)]
        tops = [[None] * 2 for t in range(tiles)]
        for j in range(cols // 8):
            line = slice(8 * j, 8 * j + 8)
            cs = cs_ref[line, :]
            for t in range(tiles):
                z = kc_ref[line, here[t]] - cs
                tops[t][j % 2] = z if j < 2 else jnp.maximum(tops[t][j % 2], z)
        tops = [jnp.max(jnp.maximum(*pair), axis=0, keepdims=True) for pair in tops]
        spans = [jnp.broadcast_to(top, (8, LANES)) for top in tops]
        sums = [[None] * 2 for t in range(tiles)]
        for j in range(cols // 8):
            line = slice(8 * j, 8 * j + 8)
            cs = cs_ref[line, :]
            for t in range(tiles):
                e = jnp.exp2(kc_ref[line, here[t]] - cs - spans[t])
                kc_ref[line, here[t]] = e
                sums[t][j % 2] = e if j < 2 else sums[t][j % 2] + e
        for t in range(tiles):
            weight = jnp.sum(sums[t][0] + sums[t][1], axis=0, keepdims=True)
            norm = norms[0:1, t * LANES : (t + 1) * LANES]
            line = pl.ds(c * tiles + t, 1)
            xs_ref[line, :] = norm
            mr_ref[line, :] = tops[t] - norm
            l_ref[line, :] = (tops[t] - norm) + log2(weight)
        return carry

    lax.fori_loop(0, rows // wide, chunk, 0)
    mass = jnp.broadcast_to(jnp.sum(cm_ref[...], axis=0, keepdims=True), (8, LANES))
    spread(out_ref, l_ref[...], mass)
    own_ref[...] = y_ref[...]
    pack_ref[0:cols, :] = y_ref[...].astype(f32)
    pack_ref[cols:, :] = jnp.zeros((pack_ref.shape[0] - cols, LANES), f32)
    pack_ref[cols : cols + cm_ref.shape[0], :] = cm_ref[...]


def widen_kernel(
    kappa, col_lines, recv_ref, x_ref, other_ref, pack_ref, xs_ref, k_ref, mr_ref, y_ref, cmb_ref, cs_ref, base_ref
):
    cols, rows = k_ref.shape
    lines = rows // LANES
    lse = joined([recv_ref[d, 0:lines, :] for d in range(recv_ref.shape[0])])
    mr_ref[...] = lse
    base_ref[...] = lse + xs_ref[...]
    y_ref[...] = other_ref[0:cols, :].astype(jnp.bfloat16)
    cs_ref[...] = jnp.broadcast_to(scaled_norms(other_ref[0:cols, :], kappa), (cols, LANES))
    cmb_ref[0:col_lines, :] = pack_ref[cols : cols + col_lines, :]
    cmb_ref[col_lines : 2 * col_lines, :] = other_ref[cols : cols + col_lines, :]
    wide = 1024
    tiles = wide // LANES

    def chunk(c, carry):
        at = pl.multiple_of(c * wide, wide)
        kc_ref = k_ref.at[:, pl.ds(at, wide)]
        kc_ref[...] = cross_of(y_ref[...], x_ref[pl.ds(at, wide), :]) * (2.0 * kappa)
        spans = [jnp.broadcast_to(base_ref[pl.ds(c * tiles + t, 1), :], (8, LANES)) for t in range(tiles)]
        for j in range(cols // 8):
            line = slice(8 * j, 8 * j + 8)
            cs = cs_ref[line, :]
            for t in range(tiles):
                across = slice(t * LANES, (t + 1) * LANES)
                kc_ref[line, across] = jnp.exp2(kc_ref[line, across] - cs - spans[t])
        return carry

    lax.fori_loop(0, rows // wide, chunk, 0)


def exact_rows(kappa, x_ref, y_refs, gcol_ref, xs_ref, l_ref):
    def chunk(c, carry):
        xb = x_ref[pl.ds(pl.multiple_of(c * LANES, LANES), LANES), :]

        def part(b, kept, y_ref, first):
            top, weight = kept
            y = y_ref[pl.ds(pl.multiple_of(b * LANES, LANES), LANES), :]
            gain = gcol_ref[pl.ds(pl.multiple_of(first + b * LANES, LANES), LANES), :]
            z = cross_of(y, xb) * (2.0 * kappa) - scaled_norms(y, kappa) + gain
            newtop = jnp.maximum(top, jnp.max(z, axis=0, keepdims=True))
            added = jnp.sum(jnp.exp2(z - newtop), axis=0, keepdims=True)
            return newtop, weight * jnp.exp2(top - newtop) + added

        kept = (jnp.full((1, LANES), -jnp.inf, f32), jnp.zeros((1, LANES), f32))
        first = 0
        for y_ref in y_refs:
            one = functools.partial(part, y_ref=y_ref, first=first)
            kept = lax.fori_loop(0, y_ref.shape[0] // LANES, one, kept)
            first += y_ref.shape[0]
        top, weight = kept
        l_ref[pl.ds(c, 1), :] = top - xs_ref[pl.ds(c, 1), :] + log2(weight)
        return carry

    lax.fori_loop(0, x_ref.shape[0] // LANES, chunk, 0)


def exact_cols(kappa, x_ref, y_ref, first, fx_ref, s_ref, top_ref, weight_ref):
    lane, sub = lane_and_sublane()

    def part(b, carry):
        y = y_ref[pl.ds(pl.multiple_of(b * LANES, LANES), LANES), :]
        top_ref[...] = jnp.full(top_ref.shape, -jnp.inf, f32)
        weight_ref[...] = jnp.zeros(weight_ref.shape, f32)

        def chunk(c, inner):
            xb = x_ref[pl.ds(pl.multiple_of(c * LANES, LANES), LANES), :]
            z = cross_of(y, xb) * (2.0 * kappa) + fx_ref[pl.ds(c, 1), :]
            top = top_ref[...]
            newtop = jnp.maximum(top, jnp.max(z, axis=1, keepdims=True))
            added = jnp.sum(jnp.exp2(z - newtop), axis=1, keepdims=True)
            weight_ref[...] = weight_ref[...] * jnp.exp2(top - newtop) + added
            top_ref[...] = newtop
            return inner

        lax.fori_loop(0, x_ref.shape[0] // LANES, chunk, 0)
        lse = top_ref[...] + log2(weight_ref[...]) - scaled_norms(y, kappa)
        line = jnp.zeros((8, LANES), f32)
        for q in range(LANES // 8):
            line = line + jnp.where(lane == sub + 8 * q, lse[8 * q : 8 * q + 8, :], 0.0)
        s_ref[pl.ds(first + b, 1), :] = jnp.sum(line, axis=0, keepdims=True)
        return carry

    lax.fori_loop(0, y_ref.shape[0] // LANES, part, 0)


def col_kernel(kappa, index, last, count, *refs):
    got, refs = refs[:count], refs[count:]
    rm_ref, fprev_ref, mr_ref, mr2_ref, xs_ref, sc_ref, errs_ref, k_ref, k2_ref, x_ref, y_ref, y2_ref, *refs = refs
    f_ref, sc_out_ref, errs_out_ref, out_ref, *refs = refs
    acc_ref, s_ref, fx_ref, top_ref, weight_ref = refs
    rows, cols = k_ref.shape[1], k_ref.shape[0]
    lines = rows // LANES
    lane, sub = lane_and_sublane()
    if index == 0:
        recv_ref = got[0]
        lse = joined([recv_ref[d, 0:lines, :] for d in range(recv_ref.shape[0])])
    else:
        lse = joined([ref[...] for ref in got])
    mass = rm_ref[...]
    la = log2(mass)
    sc = sc_ref[...]
    errs = errs_ref[...]
    if index == 0:
        f_new = la - lse
        mass_b = total(jnp.sum(recv_ref[:, lines : lines + 1, :], axis=0))
        sc = jnp.where(sub == 1, mass_b, 0.0)
        u = [f_new + ref[...] for ref in (mr_ref, mr2_ref)]
        newest = [largest(part) for part in u]
        high = newest
    else:
        mass_a = sc[0:1, :]
        shift = log2(mass_a)
        f_new = la - shift - lse
        u = [f_new + ref[...] for ref in (mr_ref, mr2_ref)]
        high = [sc[2:3, :], sc[4:5, :]]
        f_old = fprev_ref[...]
        share = mass / mass_a
        if index == 1:
            errs = noted(errs, 0, jnp.abs(jnp.exp2(la - f_old) - share))
            f_old = f_old - shift
            high = [part - shift for part in high]
        errs = noted(errs, index, jnp.abs(jnp.exp2(la - shift + (f_old - f_new)) - share))
        newest = [largest(part) for part in u]
    together = 16 if cols % 128 == 0 else 8
    for half, matrix in enumerate((k_ref, k2_ref)):
        weights = jnp.exp2(u[half] - high[half])
        us = [jnp.broadcast_to(weights[l : l + 1, :], (8, LANES)) for l in range(lines)]

        def group(t, carry, us=us, matrix=matrix, first=half * cols):
            for q in range(together):
                line = pl.ds(pl.multiple_of((t * together + q) * 8, 8), 8)
                parts = [None] * 2
                for l in range(lines):
                    term = matrix[line, l * LANES : (l + 1) * LANES] * us[l]
                    parts[l % 2] = term if parts[l % 2] is None else parts[l % 2] + term
                acc_ref[pl.ds(pl.multiple_of(first + (t * together + q) * 8, 8), 8), :] = parts[0] + parts[1]
            return carry

        lax.fori_loop(0, cols // (8 * together), group, 0)
    for t in range(2 * cols // LANES):
        picked = []
        for q in range(LANES // 8):
            at = t * LANES + 8 * q
            full = jnp.sum(acc_ref[at : at + 8, :], axis=1, keepdims=True)
            picked.append(jnp.where(lane == sub + 8 * q, full, 0.0))
        s_ref[t : t + 1, :] = jnp.sum(in_pairs(picked, jnp.add), axis=0, keepdims=True)
    sums = s_ref[...]
    extra = None
    if index == 0:
        extra = jnp.broadcast_to(jnp.sum(mass, axis=0, keepdims=True), (8, LANES))
    elif last:
        extra = jnp.broadcast_to(along_lanes(errs), (8, LANES))
    own = lax.broadcasted_iota(jnp.int32, sums.shape, 0) < cols // LANES
    spread(out_ref, jnp.where(own, high[0], high[1]) + log2(sums), extra)
    f_ref[...] = f_new * (eps / LOG2E) if last else f_new
    sc_out_ref[...] = jnp.where(sub == 2, newest[0], jnp.where(sub == 4, newest[1], sc))
    errs_out_ref[...] = errs
    drift = jnp.maximum(newest[0] - high[0], newest[1] - high[1])
    least = jnp.min(jnp.where(drift <= DRIFT, sums, 0.0))

    @pl.when(jnp.logical_not(least >= SMALLEST))
    def _():
        fx_ref[...] = f_new - xs_ref[...]
        exact_cols(kappa, x_ref, y_ref, 0, fx_ref, s_ref, top_ref, weight_ref)
        exact_cols(kappa, x_ref, y2_ref, cols // LANES, fx_ref, s_ref, top_ref, weight_ref)
        spread(out_ref, s_ref[...], extra)


def new_target(index, recv_ref, cm_ref, gprev_ref, sc, errs_ref):
    lines = cm_ref.shape[0]
    lane, sub = lane_and_sublane()
    lse = joined([recv_ref[d, 0:lines, :] for d in range(recv_ref.shape[0])])
    mass_b = sc[1:2, :]
    if index == 0:
        mass_a = total(jnp.sum(recv_ref[:, lines : lines + 1, :], axis=0))
        lse = lse - log2(mass_a)
        sc = jnp.where(sub == 0, mass_a, sc)
    mass = cm_ref[...]
    lb = log2(mass) - log2(mass_b)
    g_new = lb - lse
    terms = jnp.abs(jnp.exp2(lb + (gprev_ref[...] - g_new)) - mass / mass_b)
    errs = noted(errs_ref[...], index, terms[0 : lines // 2, :])
    return g_new, sc, errs


def row_kernel(
    kappa, index,
    recv_ref, cm_ref, gprev_ref, mr_ref, mr2_ref, xs_ref, sc_ref, errs_ref, k_ref, k2_ref, x_ref, y_ref, y2_ref,
    g_ref, sc_out_ref, errs_out_ref, out_ref,
    vbc_ref, r_ref, l_ref,
):
    rows, cols = k_ref.shape[1], k_ref.shape[0]
    lines = rows // LANES
    lane, sub = lane_and_sublane()
    sc = sc_ref[...]
    g_new, sc, errs = new_target(index, recv_ref, cm_ref, gprev_ref, sc, errs_ref)
    newest = largest(g_new)
    high = newest if index == 0 else sc[3:4, :]

    def put(at, piece):
        vbc_ref[at : at + 8, :] = piece

    column_form(jnp.exp2(g_new - high), put)
    together, block = min(16, lines), 64

    for half, matrix in enumerate((k_ref, k2_ref)):
        for first in range(0, lines, together):

            def group(b, acc, first=first, matrix=matrix, start=half * cols):
                acc = list(acc)
                for j in range(block // 8):
                    line = pl.ds(pl.multiple_of(b * block + 8 * j, 8), 8)
                    vj = vbc_ref[pl.ds(pl.multiple_of(start + b * block + 8 * j, 8), 8), :]
                    for t in range(together):
                        across = slice((first + t) * LANES, (first + t + 1) * LANES)
                        acc[t] = acc[t] + matrix[line, across] * vj
                return tuple(acc)

            acc = lax.fori_loop(0, cols // block, group, (jnp.zeros((8, LANES), f32),) * together)
            for t in range(together):
                at = half * lines + first + t
                r_ref[at : at + 1, :] = jnp.sum(acc[t], axis=0, keepdims=True)
    sums = [r_ref[0:lines, :], r_ref[lines : 2 * lines, :]]
    out_ref[...] = joined([ref[...] + (high + log2(part)) for ref, part in zip((mr_ref, mr2_ref), sums)])
    g_ref[...] = g_new
    sc_out_ref[...] = jnp.where(sub == 3, newest, sc)
    errs_out_ref[...] = errs
    least = jnp.min(jnp.where(newest - high <= DRIFT, jnp.minimum(*sums), 0.0))

    @pl.when(jnp.logical_not(least >= SMALLEST))
    def _():
        column_form(g_new, put)
        exact_rows(kappa, x_ref, (y_ref, y2_ref), vbc_ref, xs_ref, l_ref)
        out_ref[...] = l_ref[...]


def last_kernel(index, recv_ref, cm_ref, gprev_ref, sc_ref, errs_ref, g_ref, row_ref, out_ref):
    lines = cm_ref.shape[0]
    g_new, sc, errs = new_target(index, recv_ref, cm_ref, gprev_ref, sc_ref[...], errs_ref)
    g_ref[...] = g_new[0 : lines // 2, :] * (eps / LOG2E)
    row_ref[...] = jnp.broadcast_to(jnp.sum(recv_ref[:, lines : lines + 1, :], axis=0), (8, LANES))
    col_errs = jnp.broadcast_to(along_lanes(errs), (8, LANES))
    for d in range(out_ref.shape[0]):
        out_ref[d] = col_errs


def on_chip():
    return pl.BlockSpec(memory_space=pltpu.VMEM)


def call(kernel, args, outs, scratch, limit, name):
    return pl.pallas_call(
        kernel,
        in_specs=[on_chip() for _ in args],
        out_specs=[on_chip() for _ in outs],
        out_shape=[jax.ShapeDtypeStruct(shape, f32) for shape in outs],
        scratch_shapes=[pltpu.VMEM(shape, f32) for shape in scratch],
        compiler_params=pltpu.CompilerParams(vmem_limit_bytes=limit),
        name=name,
    )(*args)


def exchange(x, axis):
    return lax.all_to_all(x, axis, split_axis=0, concat_axis=0, tiled=True)


def swapped(x, by):
    count = lax.axis_size(COLS_OVER)
    return lax.ppermute(x, COLS_OVER, [(i, i ^ by) for i in range(count)])


def paired(x):
    both = joined([x, swapped(x, 1)])
    return (both, *(swapped(both, by) for by in range(2, lax.axis_size(COLS_OVER) // 2, 2)))


def on_device(row_embed, col_embed, row_mass, col_mass):
    rows, width = row_embed.shape
    cols = col_embed.shape[0]
    kappa = LOG2E / (width * eps)
    row_lines, col_lines = rows // LANES, cols // LANES
    by_col = lax.axis_size(COLS_OVER)
    by_row = lax.axis_size(ROWS_OVER)
    rm = row_mass.reshape(row_lines, LANES)
    cm = col_mass.reshape(col_lines, LANES)
    tile = (8, LANES)
    mib = 1 << 20
    shapes = [
        ((cols, rows), f32), ((row_lines, LANES), f32), ((row_lines, LANES), f32),
        ((by_col, row_lines + 8, LANES), f32), (col_embed.shape, col_embed.dtype),
        ((cols + col_lines + -col_lines % 8, LANES), f32),
    ]
    k, mr, xs, out, col_embed, pack = pl.pallas_call(
        functools.partial(init_kernel, kappa),
        in_specs=[on_chip() for _ in range(3)],
        out_specs=[on_chip() for _ in shapes],
        out_shape=[jax.ShapeDtypeStruct(*shape) for shape in shapes],
        scratch_shapes=[pltpu.VMEM((cols, LANES), f32), pltpu.VMEM((row_lines, LANES), f32)],
        compiler_params=pltpu.CompilerParams(vmem_limit_bytes=24 * mib),
        name="init",
    )(row_embed, col_embed, cm)
    other = swapped(pack, by_col // 2)
    f_pot = jnp.zeros((row_lines, LANES), f32)
    g_pot = jnp.zeros((2 * col_lines, LANES), f32)
    sc = jnp.zeros(tile, f32)
    noting = (16, LANES)
    row_errs = jnp.zeros(noting, f32)
    col_errs = jnp.zeros(noting, f32)
    vmem = pltpu.VMEM
    for index in range(ITERS):
        last = index == ITERS - 1
        if index == 0:
            got = (exchange(out, COLS_OVER),)
            k2, mr2, y2, cmb = pl.pallas_call(
                functools.partial(widen_kernel, kappa, col_lines),
                in_specs=[on_chip() for _ in range(5)],
                out_specs=[on_chip() for _ in range(4)],
                out_shape=[
                    jax.ShapeDtypeStruct((cols, rows), f32),
                    jax.ShapeDtypeStruct((row_lines, LANES), f32),
                    jax.ShapeDtypeStruct(col_embed.shape, col_embed.dtype),
                    jax.ShapeDtypeStruct((2 * col_lines, LANES), f32),
                ],
                scratch_shapes=[vmem((cols, LANES), f32), vmem((row_lines, LANES), f32)],
                compiler_params=pltpu.CompilerParams(vmem_limit_bytes=24 * mib),
                name="widen",
            )(got[0], row_embed, other, pack, xs)
        else:
            got = paired(out)
        more = 8 if index == 0 or last else 0
        fixed = (k, k2, row_embed, col_embed, y2)
        f_pot, sc, row_errs, out = call(
            functools.partial(col_kernel, kappa, index, last, len(got)),
            (*got, rm, f_pot, mr, mr2, xs, sc, row_errs, *fixed),
            [(row_lines, LANES), tile, noting, (by_row, 2 * col_lines + more, LANES)],
            [(2 * cols, LANES), (2 * col_lines, LANES), (row_lines, LANES), (LANES, LANES), (LANES, LANES)],
            24 * mib, f"cols{index}",
        )
        got = exchange(out, ROWS_OVER)
        if last:
            break
        g_pot, sc, col_errs, out = call(
            functools.partial(row_kernel, kappa, index),
            (got, cmb, g_pot, mr, mr2, xs, sc, col_errs, *fixed),
            [(2 * col_lines, LANES), tile, noting, (row_lines, LANES)],
            [(2 * cols, LANES), (2 * row_lines, LANES), (row_lines, LANES)],
            24 * mib, f"rows{index}",
        )
    g_out, row_errs, out = call(
        functools.partial(last_kernel, ITERS - 1),
        (got, cmb, g_pot, sc, col_errs),
        [(col_lines, LANES), tile, (by_col, 8, LANES)],
        [], 8 * mib, "finish",
    )
    got, row_errs = lax.optimization_barrier((exchange(out, COLS_OVER), row_errs))
    col_vec = jnp.sum(got[:, 0, :ITERS], axis=0)
    errors = jnp.stack([row_errs[0, :ITERS], col_vec], axis=1)
    return f_pot.reshape(rows), g_out.reshape(cols), errors


def solution(mesh):
    return jax.shard_map(
        on_device,
        mesh=mesh,
        in_specs=(P(ROWS_OVER, None), P(COLS_OVER, None), P(ROWS_OVER), P(COLS_OVER)),
        out_specs=(P(ROWS_OVER), P(COLS_OVER), P()),
        check_vma=False,
    )
```
